32 devices in a mesh: curve: 8 (over z, x), grp: 4 (over y, core).
Axes of the slice: x: 2, y: 2, z: 4, core: 2. Of those that a mesh axis runs over, the one named last changes fastest.
Arguments:
- state: float32 [2, 512, 4, 12288], P(None, None, 'grp', 'curve'), may hold values from -6 to 6
- coef: float32 [512, 4, 12288], P(None, 'grp', 'curve'), may hold values from 0.2 to 4
- counts: int32 [4, 8], P('grp', 'curve'), may hold values from 512 to 1536, as said below
Outputs:
- smoothed: float32 [512, 4, 8192], P(None, 'grp', 'curve')
The draws below stay inside these ranges and needn't reach their ends.
Inputs may be any that keep to these rules, and one draw needn't show every extreme that they name: `counts`: each rank's count is 1024 plus the drift at its own end minus the drift at the end of the rank before it; drifts lie in -256 to 256, are zero before the first rank and at the last rank, so the curve holds 8192 blocks; in every curve one rank holds exactly 1536 blocks.
All inputs are finite; a program needn't handle non-finite values.
Results may differ from the reference program's by a relative error of at most 0.00002.
Values sent between devices are 32-bit elements; how exact they have to be, the bound alone decides.
A program may use at most 128 MiB of HBM per device.

```python
import math
import jax
import jax.numpy as jnp

AVG = 1024
HALF = 256
CAP = 1536
SWEEPS = 2
N_CURVE = 8
N_GRP = 4


def draw_counts(key, part):
    key_walk, key_peak = jax.random.split(jax.random.fold_in(key, 11))
    drift = jax.random.randint(key_walk, (N_GRP, N_CURVE), -HALF, HALF + 1)
    peak = jax.random.randint(key_peak, (N_GRP, 1), 1, N_CURVE - 1)
    column = jnp.arange(N_CURVE, dtype=jnp.int32)[None, :]
    drift = jnp.where(column == peak, HALF, jnp.where(column == peak - 1, -HALF, drift))
    drift = jnp.where(column == N_CURVE - 1, 0, drift)
    before = jnp.concatenate([jnp.zeros((N_GRP, 1), jnp.int32), drift[:, :-1]], axis=1)
    return (AVG + drift - before).astype(jnp.int32)


def block_scale(stream_key, extent, pieces, smallest, high):
    loudness, own = 1.0, jax.random.fold_in(stream_key, 6)
    for axis_at, shards_of in pieces:
        draws = jnp.exp(jax.random.uniform(jax.random.fold_in(own, axis_at), (shards_of,), jnp.float32, smallest / len(pieces), high / len(pieces)))
        loudness = loudness * jnp.repeat(draws, extent[axis_at] // shards_of).reshape([-1 if axis == axis_at else 1 for axis in range(len(extent))])
    return loudness


def gaussian(key, dims, scale, limit, pieces=(), held_as=jnp.bfloat16):
    level = block_scale(key, dims, pieces, -0.22, 0.18) if pieces else 1.0
    values = jax.random.normal(key, dims, jnp.float32) * scale * level
    return jnp.minimum(jnp.maximum(values, -limit), limit).astype(held_as)


def setup_inputs(seed: int = 0) -> dict:
    key_list = jax.random.split(jax.random.key(seed), 4)
    return {
        "state": gaussian(key_list[0], (2, 512, N_GRP, N_CURVE * CAP), 1.0, 6.0, ((2, 4), (3, 8)), jnp.float32),
        "coef": jnp.clip(jnp.exp(math.log(4.0) - 2.9957323 * jax.random.uniform(key_list[1], (512, N_GRP, N_CURVE * CAP), jnp.float32) ** block_scale(key_list[1], (512, N_GRP, N_CURVE * CAP), ((1, 4), (2, 8)), -0.2, 0.2)), 0.2, 4.0),
        "counts": draw_counts(jax.random.fold_in(key_list[3], 71), 0),
    }


def smooth(field, source, coef, left_block, right_block, low_face, high_face):
    xplus = jnp.concatenate([field[1:], jnp.concatenate([field[0:1, :, :, :, 1:], right_block[0:1]], axis=4)], axis=0)
    xminus = jnp.concatenate([jnp.concatenate([left_block[7:8], field[7:8, :, :, :, :-1]], axis=4), field[:-1]], axis=0)
    yplus = jnp.concatenate([field[:, 1:], high_face[:, None]], axis=1)
    yminus = jnp.concatenate([low_face[:, None], field[:, :-1]], axis=1)
    zeroes = jnp.zeros_like(field[:, :, 0:1])
    zplus = jnp.concatenate([field[:, :, 1:], zeroes], axis=2)
    zminus = jnp.concatenate([zeroes, field[:, :, :-1]], axis=2)
    total = xplus + xminus + yplus + yminus + zplus + zminus
    return (source + total) / (6.0 + coef)


def reference(state, coef, counts):
    prefix = jnp.cumsum(counts, axis=1) - counts
    blocks = N_CURVE * AVG
    target = jnp.arange(blocks, dtype=jnp.int32)
    owner = jnp.sum((prefix[:, None, :] <= target[None, :, None]).astype(jnp.int32), axis=2) - 1
    start = jnp.take_along_axis(prefix, owner, axis=1)
    source_col = (owner * CAP + target[None, :] - start).astype(jnp.int32)
    moved = jnp.take_along_axis(state, jnp.broadcast_to(source_col[None, None], (2, 512, N_GRP, blocks)), axis=3)
    moved_coef = jnp.take_along_axis(coef, jnp.broadcast_to(source_col[None], (512, N_GRP, blocks)), axis=2)
    field = moved[0].reshape(8, 8, 8, N_GRP, blocks)
    source = moved[1].reshape(8, 8, 8, N_GRP, blocks)
    cellcoef = moved_coef.reshape(8, 8, 8, N_GRP, blocks)
    edge = jnp.zeros((8, 8, 8, N_GRP, 1), jnp.float32)
    plane = jnp.zeros((8, 8, 1, blocks), jnp.float32)
    for sweep in range(SWEEPS):
        low_face = jnp.concatenate([plane, field[:, 7, :, :-1, :]], axis=2)
        high_face = jnp.concatenate([field[:, 0, :, 1:, :], plane], axis=2)
        field = smooth(field, source, cellcoef, edge, edge, low_face, high_face)
    return field.reshape(512, N_GRP, blocks)
```

```python
import functools

import jax
import jax.numpy as jnp
from jax import lax
from jax.experimental import pallas as pl
from jax.experimental.pallas import tpu as pltpu
from jax.sharding import PartitionSpec as P

AVG = 1024
HALF = 256
LANES = 128
SIDE = 8
WIN = HALF // LANES
OWN = AVG // LANES
PAD = 16
FIELD, FACTOR, MIDDLE, FINAL = 0, 2 * SIDE, 6 * SIDE, 8 * SIDE
UNITS = 16 * SIDE
KINDS = 6 + SIDE
MESH = pl.DeviceIdType.MESH


def exchange(
    n, groups, rows, counts, state, coef, out, mine, every, every_s, ends, met, raw0, raw1, raw2, inverse, first,
    second, put, got, face0, face1, near0, near1, inv, fix, change, kept, edge_out, edge_in, count_send, count_recv,
    end_send, end_recv, local_sem, load_sem, send_sem, recv_sem, face_send, face_recv, edge_send, edge_recv,
):
    plane_rows = SIDE * SIDE * rows
    cells_rows = SIDE * plane_rows
    rank, group = lax.axis_index("curve"), lax.axis_index("grp")
    has_left, has_right = rank > 0, rank < n - 1
    has_low, has_high = group > 0, group < groups - 1
    sides = (
        (has_left, {"curve": rank - 1}), (has_right, {"curve": rank + 1}),
        (has_low, {"grp": group - 1}), (has_high, {"grp": group + 1}),
    )
    theres = (has_low, has_high)
    raw = (raw0, raw1, raw2)
    front = (plane_rows, 0, 0)
    loads = {}
    for f, src in ((0, state.at[0]), (2, coef), (1, state.at[1])):
        loads[f] = pltpu.make_async_copy(src, raw[f].at[pl.ds(front[f], cells_rows)], load_sem.at[f])
        loads[f].start()
    barrier = pltpu.get_barrier_semaphore()
    for there, device in sides:
        @pl.when(there)
        def _():
            pl.semaphore_signal(barrier, inc=1, device_id=device, device_id_type=MESH)
    for off in range(2, n - 1):
        peer = lax.rem(rank + off, n)
        pl.semaphore_signal(barrier, inc=1, device_id={"curve": peer}, device_id_type=MESH)
    for there, peer in ((has_left, n - 1), (has_right, 0)):
        @pl.when(jnp.logical_not(there))
        def _():
            pl.semaphore_signal(barrier, inc=1, device_id={"curve": peer}, device_id_type=MESH)

    lane = lax.broadcasted_iota(jnp.int32, (SIDE, LANES), 1)
    level = lax.broadcasted_iota(jnp.int32, (SIDE, LANES), 0)
    held = jnp.clip(counts[0, 0], 2 * HALF, rows * LANES)
    mine[...] = jnp.full((1, LANES), held, jnp.int32)
    last = held - 1
    last_row, last_lane = lax.shift_right_logical(last, 7), last & (LANES - 1)
    tail_row = lax.shift_right_logical(held, 7) - WIN
    tail_part = held & (LANES - 1)
    tail_turn = (LANES - tail_part) & (LANES - 1)
    tail_stay = lane >= tail_part

    def raw_at(f, x, y, r):
        return pl.ds(front[f] + (x * SIDE + y) * (SIDE * rows) + r, SIDE, stride=rows)

    def field_of(x, y, r):
        return raw0[raw_at(0, x, y, r), :]

    def first_at(x, y, r):
        return pl.ds((((x + 1) * SIDE + y) * rows + r) * SIDE, SIDE)

    def flat_at(x, y, r):
        return pl.ds(PAD + ((x * SIDE + y) * rows + r) * SIDE, SIDE)

    def factor_of(x, y, r):
        return 1.0 / (raw2[raw_at(2, x, y, r), :] + 6.0)

    def pack(unit, get, x, y):
        for i in range(WIN):
            put[0, unit, i] = get(x, y, i)
        lines = [get(x, y, tail_row + i) for i in range(WIN + 1)]
        for i in range(WIN):
            put[1, unit, i] = pltpu.roll(jnp.where(tail_stay, lines[i], lines[i + 1]), tail_turn, 1)

    def message(kind):
        if kind < 2:
            return FIELD + kind * SIDE, SIDE
        if kind < 4:
            return FACTOR + (kind - 2) * 2 * SIDE, 2 * SIDE
        if kind < 6:
            return MIDDLE + (kind - 4) * SIDE, SIDE
        return FINAL + (kind - 6) * SIDE, SIDE

    def sent(kind, side):
        start, count = message(kind)
        return pltpu.make_async_remote_copy(
            src_ref=put.at[side, pl.ds(start, count)], dst_ref=got.at[1 - side, pl.ds(start, count)],
            send_sem=send_sem.at[side * KINDS + kind], recv_sem=recv_sem.at[side * KINDS + kind],
            device_id=sides[side][1], device_id_type=MESH,
        )

    def needed(kind, side):
        return sides[side][0] & theres[kind % 2] if kind < 6 else sides[side][0]

    def send(kind):
        for side in range(2):
            @pl.when(needed(kind, side))
            def _():
                sent(kind, side).start()

    def arrived(kind):
        for side in range(2):
            @pl.when(needed(kind, side))
            def _():
                sent(kind, 1 - side).wait_recv()

    outer, inner = (0, SIDE - 1), (1, SIDE - 2)
    loads[0].wait()
    @pl.loop(0, SIDE)
    def _(x):
        for p in range(2):
            pack(FIELD + p * SIDE + x, field_of, x, outer[p])
    loads[2].wait()
    @pl.loop(0, SIDE)
    def _(x):
        for p in range(2):
            for k, y in enumerate((outer[p], inner[p])):
                pack(FACTOR + (2 * p + k) * SIDE + x, factor_of, x, y)
    loads[1].wait()
    for side, at, turn, outer_x, near_x in ((0, 0, 0, 1, 0), (1, last_row, LANES - last_lane, SIDE - 2, SIDE - 1)):
        packed = jnp.zeros((SIDE, LANES), jnp.float32)
        for p, (f, x) in enumerate(((0, outer_x), (0, near_x), (1, near_x), (2, near_x))):
            for y in range(SIDE):
                value = factor_of(x, y, at) if f == 2 else raw[f][raw_at(f, x, y, at), :]
                spot = p * SIDE + y
                value = pltpu.roll(value, (turn + spot) & (LANES - 1), 1)
                packed = jnp.where(lane == spot, value, packed)
        ends[side] = packed

    pl.semaphore_wait(barrier, n - 1 + has_low.astype(jnp.int32) + has_high.astype(jnp.int32))

    def greeted(side):
        return pltpu.make_async_remote_copy(
            src_ref=ends.at[side], dst_ref=met.at[1 - side], send_sem=end_send.at[side],
            recv_sem=end_recv.at[side], device_id=sides[side][1], device_id_type=MESH,
        )

    for side in range(2):
        @pl.when(sides[side][0])
        def _():
            greeted(side).start()
    tallies = []
    for off in range(1, n):
        tallies.append(
            pltpu.make_async_remote_copy(
                src_ref=mine, dst_ref=every.at[rank], send_sem=count_send.at[off],
                recv_sem=count_recv.at[off], device_id={"curve": lax.rem(rank + off, n)},
                device_id_type=MESH,
            )
        )
        tallies[-1].start()
    keep = pltpu.make_async_copy(mine, every.at[rank], local_sem.at[0])
    keep.start()
    for kind in range(4):
        send(kind)

    for side in range(2):
        @pl.when(sides[side][0])
        def _():
            greeted(1 - side).wait_recv()
    shown = [ends[side] for side in range(2)]
    seen = [jnp.where(sides[side][0], met[side], 0.0) for side in range(2)]

    def sums(value):
        above = jnp.where(level < SIDE - 1, pltpu.roll(value, SIDE - 1, 0), 0.0)
        return above + jnp.where(level > 0, pltpu.roll(value, 1, 0), 0.0)

    def borders(get, store, ghosts, spot):
        @pl.loop(0, SIDE // 2)
        def _(half):
            for y in (2 * half, 2 * half + 1):
                turned = [pltpu.roll(get(SIDE - 1, y, r), 1, 1) for r in range(rows)]
                carry = pltpu.roll(ghosts[0], (LANES - spot - y) & (LANES - 1), 1)
                for r in range(rows):
                    store(-1, y, r, jnp.where(lane == 0, carry, turned[r]))
                    carry = turned[r]
                turned = [pltpu.roll(get(0, y, r), LANES - 1, 1) for r in range(rows)]
                ghost = pltpu.roll(ghosts[1], (last_lane + LANES - spot - y) & (LANES - 1), 1)
                for r in range(rows):
                    value = jnp.where(lane == LANES - 1, turned[r + 1], turned[r]) if r + 1 < rows else turned[r]
                    store(SIDE, y, r, jnp.where(lane + r * LANES == last, ghost, value))

    def sweep(get, factor, store):
        @pl.loop(0, SIDE)
        def _(x):
            for r in range(rows):
                line = [get(x, y, r) for y in range(SIDE)]
                for y in range(SIDE):
                    total = (get(x - 1, y, r) + get(x + 1, y, r)) + (raw1[raw_at(1, x, y, r), :] + sums(line[y]))
                    if y > 0:
                        total = total + line[y - 1]
                    if y + 1 < SIDE:
                        total = total + line[y + 1]
                    store(x, y, r, total * factor(x, y, r))

    def store_field(x, y, r, value):
        raw0[raw_at(0, x, y, r), :] = value

    def first_of(x, y, r):
        return first[first_at(x, y, r), :]

    def store_first(x, y, r, value):
        first[first_at(x, y, r), :] = value

    def made_factor(x, y, r):
        value = factor_of(x, y, r)
        inverse[flat_at(x, y, r), :] = value
        return value

    def inverse_of(x, y, r):
        return inverse[flat_at(x, y, r), :]

    def second_of(x, y, r):
        return second[flat_at(x, y, r), :]

    def store_second(x, y, r, value):
        second[flat_at(x, y, r), :] = value

    borders(field_of, store_field, seen, SIDE)
    sweep(field_of, made_factor, store_first)
    @pl.loop(0, SIDE)
    def _(x):
        for p in range(2):
            pack(MIDDLE + p * SIDE + x, first_of, x, outer[p])
    for kind in range(4, 6):
        send(kind)

    def moved(met_end, own_end):
        near = pltpu.roll(met_end, LANES - SIDE, 1)
        total = met_end + pltpu.roll(own_end, LANES - SIDE, 1) + sums(near)
        total = total + jnp.where(lane < SIDE - 1, pltpu.roll(near, LANES - 1, 1), 0.0)
        total = total + jnp.where(lane > 0, pltpu.roll(near, 1, 1), 0.0)
        total = total + pltpu.roll(met_end, LANES - 2 * SIDE, 1)
        return total * pltpu.roll(met_end, LANES - 3 * SIDE, 1)

    seen = [moved(seen[side], shown[side]) for side in range(2)]
    borders(first_of, store_first, seen, 0)
    sweep(first_of, inverse_of, store_second)
    @pl.loop(0, SIDE)
    def _(x):
        for y in range(SIDE):
            pack(FINAL + x * SIDE + y, second_of, x, y)
    for kind in range(6, KINDS):
        send(kind)

    keep.wait()
    for copy in tallies:
        copy.wait()
    keep = pltpu.make_async_copy(every, every_s, local_sem.at[1])
    keep.start()
    keep.wait()
    before = 0
    for r in range(n):
        before = before + jnp.where(r < rank, every_s[r, 0, 0], 0)
    drift_prev = jnp.clip(before - rank * AVG, -HALF, HALF)
    drift_next = jnp.clip(drift_prev + held - AVG, -HALF, HALF)
    base = lax.shift_right_arithmetic(-drift_prev, 7)
    part = (-drift_prev) & (LANES - 1)
    turn = (LANES - part) & (LANES - 1)
    stay = lane >= part
    shift = HALF - jnp.maximum(drift_prev, 0)
    left_part = shift & (LANES - 1)
    left_turn = (LANES - left_part) & (LANES - 1)
    left_pick = (lane >= left_part) & (shift < LANES)
    shift = -HALF - jnp.minimum(drift_next, 0)
    right_part = shift & (LANES - 1)
    right_turn = (LANES - right_part) & (LANES - 1)
    right_pick = (lane < right_part + jnp.where(shift == 0, LANES, 0)) & (shift >= -LANES)
    is_left = [lane + i * LANES < drift_prev for i in range(WIN)]
    is_right = [lane + i * LANES >= HALF + drift_next for i in range(WIN)]

    def aligned(get, x, y):
        lines = [get(x, y, base + i) for i in range(OWN + 1)]
        return [pltpu.roll(jnp.where(stay, lines[i], lines[i + 1]), turn, 1) for i in range(OWN)]

    def windows(unit):
        low, high = got[0, unit, 0], got[0, unit, 1]
        a = [pltpu.roll(jnp.where(left_pick, low, high), left_turn, 1), pltpu.roll(high, left_turn, 1)]
        low, high = got[1, unit, 0], got[1, unit, 1]
        b = [pltpu.roll(low, right_turn, 1), pltpu.roll(jnp.where(right_pick, high, low), right_turn, 1)]
        return a, b

    def merged(get, x, y, unit):
        lines = aligned(get, x, y)
        a, b = windows(unit)
        for i in range(WIN):
            lines[i] = jnp.where(is_left[i], a[i], lines[i])
            lines[OWN - WIN + i] = jnp.where(is_right[i], b[i], lines[OWN - WIN + i])
        return lines

    def face(b, p):
        src, dst = ((face0, near0), (face1, near1))[b]
        return pltpu.make_async_remote_copy(
            src_ref=src.at[p], dst_ref=dst.at[1 - p], send_sem=face_send.at[2 * b + p],
            recv_sem=face_recv.at[2 * b + p], device_id=sides[2 + p][1], device_id_type=MESH,
        )

    def edge(side, p):
        return pltpu.make_async_remote_copy(
            src_ref=edge_out.at[side, p], dst_ref=edge_in.at[1 - side, p], send_sem=edge_send.at[2 * side + p],
            recv_sem=edge_recv.at[2 * side + p], device_id=sides[side][1], device_id_type=MESH,
        )

    for p in range(2):
        arrived(p)
        @pl.when(theres[p])
        def _():
            @pl.loop(0, SIDE // 2)
            def _(half):
                for x in (2 * half, 2 * half + 1):
                    lines = merged(field_of, x, outer[p], FIELD + p * SIDE + x)
                    for i in range(OWN):
                        face0[p, x, i] = lines[i]
            face(0, p).start()
    for p in range(2):
        arrived(2 + p)
        @pl.when(theres[p])
        def _():
            @pl.loop(0, SIDE)
            def _(x):
                for k, y in enumerate((outer[p], inner[p])):
                    lines = merged(inverse_of, x, y, FACTOR + (2 * p + k) * SIDE + x)
                    for i in range(OWN):
                        inv[p, k, x, i] = lines[i]

        @pl.when(jnp.logical_not(theres[p]))
        def _():
            @pl.loop(0, SIDE)
            def _(x):
                for k in range(2):
                    for i in range(OWN):
                        change[p, k, x, i] = jnp.zeros((SIDE, LANES), jnp.float32)
    for p in range(2):
        @pl.when(theres[p])
        def _():
            face(0, 1 - p).wait_recv()
            @pl.loop(0, SIDE)
            def _(x):
                for i in range(OWN):
                    value = near0[p, x, i] * inv[p, 0, x, i]
                    fix[p, x + 1, i] = value
                    change[p, 1, x, i] = value * inv[p, 1, x, i]
            turned = [pltpu.roll(fix[p, 1, i], LANES - 1, 1) for i in range(OWN)]
            edge_out[0, p] = turned[0]
            for i in range(OWN):
                fix[p, SIDE + 1, i] = jnp.where(lane == LANES - 1, turned[i + 1], turned[i]) if i + 1 < OWN else turned[i]
            turned = [pltpu.roll(fix[p, SIDE, i], 1, 1) for i in range(OWN)]
            edge_out[1, p] = turned[OWN - 1]
            for i in range(OWN):
                fix[p, 0, i] = jnp.where(lane == 0, turned[i - 1], turned[i]) if i else turned[i]
            for side in range(2):
                @pl.when(sides[side][0])
                def _():
                    edge(side, p).start()
    for p in range(2):
        arrived(4 + p)
        @pl.when(theres[p])
        def _():
            @pl.loop(0, SIDE // 2)
            def _(half):
                for x in (2 * half, 2 * half + 1):
                    lines = merged(first_of, x, outer[p], MIDDLE + p * SIDE + x)
                    for i in range(OWN):
                        face1[p, x, i] = lines[i] + fix[p, x + 1, i]
            face(1, p).start()
    for p in range(2):
        @pl.when(theres[p])
        def _():
            for side, x, i, spot in ((0, 0, 0, 0), (1, SIDE + 1, OWN - 1, LANES - 1)):
                @pl.when(sides[side][0])
                def _():
                    edge(1 - side, p).wait_recv()
                value = jnp.where(sides[side][0], edge_in[side, p], 0.0)
                fix[p, x, i] = jnp.where(lane == spot, value, fix[p, x, i])
            face(1, 1 - p).wait_recv()
            @pl.loop(0, SIDE)
            def _(x):
                for i in range(OWN):
                    total = near1[p, x, i] + (fix[p, x, i] + fix[p, x + 2, i]) + sums(fix[p, x + 1, i])
                    change[p, 0, x, i] = total * inv[p, 0, x, i]

    def at(x, y, i):
        return pl.ds((x * SIDE + y) * (SIDE * OWN) + i, SIDE, stride=OWN)

    spots = {0: (0, 0), 1: (0, 1), SIDE - 2: (1, 1), SIDE - 1: (1, 0)}
    window = [i for i in range(OWN) if i < WIN or i >= OWN - WIN]

    @pl.loop(0, SIDE)
    def _(x):
        for y in range(SIDE):
            lines = aligned(second_of, x, y)
            for i in range(OWN):
                if i in window:
                    kept[x, y, window.index(i)] = lines[i]
                elif y in spots:
                    out[at(x, y, i), :] = lines[i] + change[spots[y][0], spots[y][1], x, i]
                else:
                    out[at(x, y, i), :] = lines[i]
    for x in range(SIDE):
        arrived(6 + x)
        for y in range(SIDE):
            a, b = windows(FINAL + x * SIDE + y)
            for j, i in enumerate(window):
                value = jnp.where(is_left[i], a[i], kept[x, y, j]) if i < WIN else jnp.where(
                    is_right[j - WIN], b[j - WIN], kept[x, y, j]
                )
                if y in spots:
                    value = value + change[spots[y][0], spots[y][1], x, i]
                out[at(x, y, i), :] = value
    for side in range(2):
        @pl.when(sides[side][0])
        def _():
            greeted(side).wait_send()
    for p in range(2):
        @pl.when(theres[p])
        def _():
            for b in range(2):
                face(b, p).wait_send()
            for side in range(2):
                @pl.when(sides[side][0])
                def _():
                    edge(side, p).wait_send()
    for kind in range(KINDS):
        for side in range(2):
            @pl.when(needed(kind, side))
            def _():
                sent(kind, side).wait_send()


def local(state, coef, counts):
    n, groups = lax.axis_size("curve"), lax.axis_size("grp")
    cells, cap = state.shape[1], state.shape[3]
    rows = cap // LANES
    plane = SIDE * SIDE * rows
    f32 = jnp.float32
    vmem, hbm, smem = (pl.BlockSpec(memory_space=m) for m in (pltpu.VMEM, pltpu.HBM, pltpu.SMEM))
    tile = (SIDE, LANES)
    shapes = [(cells * rows + 2 * plane, LANES), (cells * rows, LANES), (cells * rows + PAD, LANES)]
    shapes += [(cells * rows + 2 * PAD, LANES), (cells * rows + 2 * plane, LANES), (cells * rows + 2 * PAD, LANES)]
    shapes += [(2, UNITS, WIN) + tile] * 2
    shapes += [(2, SIDE, OWN) + tile] * 4
    shapes += [(2, 2, SIDE, OWN) + tile, (2, SIDE + 2, OWN) + tile, (2, 2, SIDE, OWN) + tile]
    shapes += [(SIDE, SIDE, 2 * WIN) + tile] + [(2, 2) + tile] * 2
    out = pl.pallas_call(
        functools.partial(exchange, n, groups, rows),
        out_shape=jax.ShapeDtypeStruct((cells * OWN, LANES), f32),
        in_specs=[smem, hbm, hbm],
        out_specs=vmem,
        scratch_shapes=[
            pltpu.VMEM((1, LANES), jnp.int32),
            pltpu.VMEM((n, 1, LANES), jnp.int32),
            pltpu.SMEM((n, 1, LANES), jnp.int32),
            pltpu.VMEM((2,) + tile, f32),
            pltpu.VMEM((2,) + tile, f32),
        ]
        + [pltpu.VMEM(shape, f32) for shape in shapes]
        + [pltpu.SemaphoreType.DMA((k,)) for k in (n, n, 2, 2, 2, 3, 2 * KINDS, 2 * KINDS, 4, 4, 4, 4)],
        compiler_params=pltpu.CompilerParams(
            collective_id=0, has_side_effects=True, vmem_limit_bytes=48 * 1024 * 1024
        ),
    )(
        counts, state.reshape(2, cells * rows, LANES), coef.reshape(cells * rows, LANES),
    )
    return out.reshape(cells, 1, AVG)


def solution(mesh):
    placed = (P(None, None, "grp", "curve"), P(None, "grp", "curve"), P("grp", "curve"))
    return jax.shard_map(
        local, mesh=mesh, in_specs=placed, out_specs=P(None, "grp", "curve"), check_vma=False
    )
```

```python
import functools

import jax
import jax.numpy as jnp
from jax import lax
from jax.experimental import pallas as pl
from jax.experimental.pallas import tpu as pltpu
from jax.sharding import PartitionSpec as P

AVG = 1024
HALF = 256
LANES = 128
SIDE = 8
WIN = HALF // LANES
OWN = AVG // LANES
PAD = 16
FIELD, FACTOR, MIDDLE, FINAL = 0, 2 * SIDE, 6 * SIDE, 8 * SIDE
UNITS = 16 * SIDE
KINDS = 6 + SIDE
MESH = pl.DeviceIdType.MESH
EARLY_ACROSS, EARLY_PAIRED = 4, 3


def exchange(
    n, groups, rows, counts, state, coef, out, mine, every, every_s, ends, met, raw0, raw1, raw2, inverse, first,
    second, put, got, face0, face1, near0, near1, inv, fix, change, kept, edge_out, edge_in, count_send, count_recv,
    end_send, end_recv, local_sem, load_sem, send_sem, recv_sem, face_send, face_recv, edge_send, edge_recv,
):
    plane_rows = SIDE * SIDE * rows
    cells_rows = SIDE * plane_rows
    rank, group = lax.axis_index("curve"), lax.axis_index("grp")
    has_left, has_right = rank > 0, rank < n - 1
    has_low, has_high = group > 0, group < groups - 1
    sides = (
        (has_left, {"curve": rank - 1}), (has_right, {"curve": rank + 1}),
        (has_low, {"grp": group - 1}), (has_high, {"grp": group + 1}),
    )
    theres = (has_low, has_high)
    raw = (raw0, raw1, raw2)
    front = (plane_rows, 0, 0)
    loads = {}
    for f, src in ((0, state.at[0]), (2, coef), (1, state.at[1])):
        loads[f] = pltpu.make_async_copy(src, raw[f].at[pl.ds(front[f], cells_rows)], load_sem.at[f])
        loads[f].start()
    barrier = pltpu.get_barrier_semaphore()
    for there, device in sides:
        @pl.when(there)
        def _():
            pl.semaphore_signal(barrier, inc=1, device_id=device, device_id_type=MESH)
    for off in range(2, n - 1):
        peer = lax.rem(rank + off, n)
        pl.semaphore_signal(barrier, inc=1, device_id={"curve": peer}, device_id_type=MESH)
    for there, peer in ((has_left, n - 1), (has_right, 0)):
        @pl.when(jnp.logical_not(there))
        def _():
            pl.semaphore_signal(barrier, inc=1, device_id={"curve": peer}, device_id_type=MESH)

    lane = lax.broadcasted_iota(jnp.int32, (SIDE, LANES), 1)
    level = lax.broadcasted_iota(jnp.int32, (SIDE, LANES), 0)
    held = jnp.clip(counts[0, 0], 2 * HALF, rows * LANES)
    mine[...] = jnp.full((1, LANES), held, jnp.int32)
    last = held - 1
    last_row, last_lane = lax.shift_right_logical(last, 7), last & (LANES - 1)
    tail_row = lax.shift_right_logical(held, 7) - WIN
    tail_part = held & (LANES - 1)
    tail_turn = (LANES - tail_part) & (LANES - 1)
    tail_stay = lane >= tail_part

    def raw_at(f, x, y, r):
        return pl.ds(front[f] + (x * SIDE + y) * (SIDE * rows) + r, SIDE, stride=rows)

    def field_of(x, y, r):
        return raw0[raw_at(0, x, y, r), :]

    def first_at(x, y, r):
        return pl.ds((((x + 1) * SIDE + y) * rows + r) * SIDE, SIDE)

    def flat_at(x, y, r):
        return pl.ds(PAD + ((x * SIDE + y) * rows + r) * SIDE, SIDE)

    def factor_of(x, y, r):
        return 1.0 / (raw2[raw_at(2, x, y, r), :] + 6.0)

    def pack(unit, get, x, y):
        for i in range(WIN):
            put[0, unit, i] = get(x, y, i)
        lines = [get(x, y, tail_row + i) for i in range(WIN + 1)]
        for i in range(WIN):
            put[1, unit, i] = pltpu.roll(jnp.where(tail_stay, lines[i], lines[i + 1]), tail_turn, 1)

    def message(kind):
        if kind < 2:
            return FIELD + kind * SIDE, SIDE
        if kind < 4:
            return FACTOR + (kind - 2) * 2 * SIDE, 2 * SIDE
        if kind < 6:
            return MIDDLE + (kind - 4) * SIDE, SIDE
        return FINAL + (kind - 6) * SIDE, SIDE

    def sent(kind, side):
        start, count = message(kind)
        return pltpu.make_async_remote_copy(
            src_ref=put.at[side, pl.ds(start, count)], dst_ref=got.at[1 - side, pl.ds(start, count)],
            send_sem=send_sem.at[side * KINDS + kind], recv_sem=recv_sem.at[side * KINDS + kind],
            device_id=sides[side][1], device_id_type=MESH,
        )

    def needed(kind, side):
        return sides[side][0] & theres[kind % 2] if kind < 6 else sides[side][0]

    paired = lax.rem(rank, 2) == 1, lax.rem(rank, 2) == 0

    def send(kind, only=(True, True)):
        for side in range(2):
            @pl.when(needed(kind, side) & only[side])
            def _():
                sent(kind, side).start()

    def arrived(kind):
        for side in range(2):
            @pl.when(needed(kind, side))
            def _():
                sent(kind, 1 - side).wait_recv()

    def spread(step, fn):
        @pl.loop(0, SIDE // step)
        def _(part):
            for at in range(step):
                fn(step * part + at)

    outer, inner = (0, SIDE - 1), (1, SIDE - 2)
    loads[0].wait()

    def step(x):
        for p in range(2):
            pack(FIELD + p * SIDE + x, field_of, x, outer[p])
    spread(4, step)
    loads[2].wait()
    loads[1].wait()
    for side, at, turn, outer_x, near_x in ((0, 0, 0, 1, 0), (1, last_row, LANES - last_lane, SIDE - 2, SIDE - 1)):
        packed = jnp.zeros((SIDE, LANES), jnp.float32)
        for p, (f, x) in enumerate(((0, outer_x), (0, near_x), (1, near_x), (2, near_x))):
            for y in range(SIDE):
                value = factor_of(x, y, at) if f == 2 else raw[f][raw_at(f, x, y, at), :]
                spot = p * SIDE + y
                value = pltpu.roll(value, (turn + spot) & (LANES - 1), 1)
                packed = jnp.where(lane == spot, value, packed)
        ends[side] = packed

    pl.semaphore_wait(barrier, n - 1 + has_low.astype(jnp.int32) + has_high.astype(jnp.int32))

    def greeted(side):
        return pltpu.make_async_remote_copy(
            src_ref=ends.at[side], dst_ref=met.at[1 - side], send_sem=end_send.at[side],
            recv_sem=end_recv.at[side], device_id=sides[side][1], device_id_type=MESH,
        )

    for side in range(2):
        @pl.when(sides[side][0])
        def _():
            greeted(side).start()
    tallies = []
    for off in range(1, n):
        tallies.append(
            pltpu.make_async_remote_copy(
                src_ref=mine, dst_ref=every.at[rank], send_sem=count_send.at[off],
                recv_sem=count_recv.at[off], device_id={"curve": lax.rem(rank + off, n)},
                device_id_type=MESH,
            )
        )
        tallies[-1].start()
    keep = pltpu.make_async_copy(mine, every.at[rank], local_sem.at[0])
    keep.start()
    for kind in range(2):
        send(kind)

    def step(x):
        for p in range(2):
            for k, y in enumerate((outer[p], inner[p])):
                pack(FACTOR + (2 * p + k) * SIDE + x, factor_of, x, y)
    spread(4, step)
    for kind in range(2, 4):
        send(kind)

    for side in range(2):
        @pl.when(sides[side][0])
        def _():
            greeted(1 - side).wait_recv()
    shown = [ends[side] for side in range(2)]
    seen = [jnp.where(sides[side][0], met[side], 0.0) for side in range(2)]

    def sums(value):
        above = jnp.where(level < SIDE - 1, pltpu.roll(value, SIDE - 1, 0), 0.0)
        return above + jnp.where(level > 0, pltpu.roll(value, 1, 0), 0.0)

    def borders(get, store, ghosts, spot):
        def step(y):
            if True:
                turned = [pltpu.roll(get(SIDE - 1, y, r), 1, 1) for r in range(rows)]
                carry = pltpu.roll(ghosts[0], (LANES - spot - y) & (LANES - 1), 1)
                for r in range(rows):
                    store(-1, y, r, jnp.where(lane == 0, carry, turned[r]))
                    carry = turned[r]
                turned = [pltpu.roll(get(0, y, r), LANES - 1, 1) for r in range(rows)]
                ghost = pltpu.roll(ghosts[1], (last_lane + LANES - spot - y) & (LANES - 1), 1)
                for r in range(rows):
                    value = jnp.where(lane == LANES - 1, turned[r + 1], turned[r]) if r + 1 < rows else turned[r]
                    store(SIDE, y, r, jnp.where(lane + r * LANES == last, ghost, value))
        spread(4, step)

    def sweep(get, factor, store):
        @pl.loop(0, SIDE)
        def _(x):
            for r in range(rows):
                line = [get(x, y, r) for y in range(SIDE)]
                for y in range(SIDE):
                    total = (get(x - 1, y, r) + get(x + 1, y, r)) + (raw1[raw_at(1, x, y, r), :] + sums(line[y]))
                    if y > 0:
                        total = total + line[y - 1]
                    if y + 1 < SIDE:
                        total = total + line[y + 1]
                    store(x, y, r, total * factor(x, y, r))

    def store_field(x, y, r, value):
        raw0[raw_at(0, x, y, r), :] = value

    def first_of(x, y, r):
        return first[first_at(x, y, r), :]

    def store_first(x, y, r, value):
        first[first_at(x, y, r), :] = value

    def made_factor(x, y, r):
        value = factor_of(x, y, r)
        inverse[flat_at(x, y, r), :] = value
        return value

    def inverse_of(x, y, r):
        return inverse[flat_at(x, y, r), :]

    def second_of(x, y, r):
        return second[flat_at(x, y, r), :]

    def store_second(x, y, r, value):
        second[flat_at(x, y, r), :] = value

    borders(field_of, store_field, seen, SIDE)
    sweep(field_of, made_factor, store_first)

    def step(x):
        for p in range(2):
            pack(MIDDLE + p * SIDE + x, first_of, x, outer[p])
    spread(4, step)
    for kind in range(4, 6):
        send(kind)

    def moved(met_end, own_end):
        near = pltpu.roll(met_end, LANES - SIDE, 1)
        total = met_end + pltpu.roll(own_end, LANES - SIDE, 1) + sums(near)
        total = total + jnp.where(lane < SIDE - 1, pltpu.roll(near, LANES - 1, 1), 0.0)
        total = total + jnp.where(lane > 0, pltpu.roll(near, 1, 1), 0.0)
        total = total + pltpu.roll(met_end, LANES - 2 * SIDE, 1)
        return total * pltpu.roll(met_end, LANES - 3 * SIDE, 1)

    seen = [moved(seen[side], shown[side]) for side in range(2)]
    borders(first_of, store_first, seen, 0)
    sweep(first_of, inverse_of, store_second)

    def step(x):
        for y in range(SIDE):
            pack(FINAL + x * SIDE + y, second_of, x, y)
    spread(2, step)
    across = [jnp.logical_not(x) for x in paired]
    for kind in range(6, KINDS):
        for only, count in ((across, EARLY_ACROSS), (paired, EARLY_PAIRED)):
            if kind - 6 < count:
                send(kind, only)

    keep.wait()
    for copy in tallies:
        copy.wait()
    keep = pltpu.make_async_copy(every, every_s, local_sem.at[1])
    keep.start()
    keep.wait()
    before = 0
    for r in range(n):
        before = before + jnp.where(r < rank, every_s[r, 0, 0], 0)
    drift_prev = jnp.clip(before - rank * AVG, -HALF, HALF)
    drift_next = jnp.clip(drift_prev + held - AVG, -HALF, HALF)
    base = lax.shift_right_arithmetic(-drift_prev, 7)
    part = (-drift_prev) & (LANES - 1)
    turn = (LANES - part) & (LANES - 1)
    stay = lane >= part
    shift = HALF - jnp.maximum(drift_prev, 0)
    left_part = shift & (LANES - 1)
    left_turn = (LANES - left_part) & (LANES - 1)
    left_pick = (lane >= left_part) & (shift < LANES)
    shift = -HALF - jnp.minimum(drift_next, 0)
    right_part = shift & (LANES - 1)
    right_turn = (LANES - right_part) & (LANES - 1)
    right_pick = (lane < right_part + jnp.where(shift == 0, LANES, 0)) & (shift >= -LANES)
    is_left = [lane + i * LANES < drift_prev for i in range(WIN)]
    is_right = [lane + i * LANES >= HALF + drift_next for i in range(WIN)]

    def aligned(get, x, y):
        lines = [get(x, y, base + i) for i in range(OWN + 1)]
        return [pltpu.roll(jnp.where(stay, lines[i], lines[i + 1]), turn, 1) for i in range(OWN)]

    def windows(unit):
        low, high = got[0, unit, 0], got[0, unit, 1]
        a = [pltpu.roll(jnp.where(left_pick, low, high), left_turn, 1), pltpu.roll(high, left_turn, 1)]
        low, high = got[1, unit, 0], got[1, unit, 1]
        b = [pltpu.roll(low, right_turn, 1), pltpu.roll(jnp.where(right_pick, high, low), right_turn, 1)]
        return a, b

    def merged(get, x, y, unit):
        lines = aligned(get, x, y)
        a, b = windows(unit)
        for i in range(WIN):
            lines[i] = jnp.where(is_left[i], a[i], lines[i])
            lines[OWN - WIN + i] = jnp.where(is_right[i], b[i], lines[OWN - WIN + i])
        return lines

    def face(b, p):
        src, dst = ((face0, near0), (face1, near1))[b]
        return pltpu.make_async_remote_copy(
            src_ref=src.at[p], dst_ref=dst.at[1 - p], send_sem=face_send.at[2 * b + p],
            recv_sem=face_recv.at[2 * b + p], device_id=sides[2 + p][1], device_id_type=MESH,
        )

    def edge(side, p):
        return pltpu.make_async_remote_copy(
            src_ref=edge_out.at[side, p], dst_ref=edge_in.at[1 - side, p], send_sem=edge_send.at[2 * side + p],
            recv_sem=edge_recv.at[2 * side + p], device_id=sides[side][1], device_id_type=MESH,
        )

    for p in range(2):
        arrived(p)
        @pl.when(theres[p])
        def _():
            def step(x):
                lines = merged(field_of, x, outer[p], FIELD + p * SIDE + x)
                for i in range(OWN):
                    face0[p, x, i] = lines[i]
            spread(4, step)
            face(0, p).start()
    for p in range(2):
        arrived(2 + p)
        @pl.when(theres[p])
        def _():
            def step(x):
                for k, y in enumerate((outer[p], inner[p])):
                    lines = merged(inverse_of, x, y, FACTOR + (2 * p + k) * SIDE + x)
                    for i in range(OWN):
                        inv[p, k, x, i] = lines[i]
            spread(4, step)

        @pl.when(jnp.logical_not(theres[p]))
        def _():
            @pl.loop(0, SIDE)
            def _(x):
                for k in range(2):
                    for i in range(OWN):
                        change[p, k, x, i] = jnp.zeros((SIDE, LANES), jnp.float32)
    for p in range(2):
        @pl.when(theres[p])
        def _():
            face(0, 1 - p).wait_recv()
            @pl.loop(0, SIDE)
            def _(x):
                for i in range(OWN):
                    value = near0[p, x, i] * inv[p, 0, x, i]
                    fix[p, x + 1, i] = value
                    change[p, 1, x, i] = value * inv[p, 1, x, i]
            turned = [pltpu.roll(fix[p, 1, i], LANES - 1, 1) for i in range(OWN)]
            edge_out[0, p] = turned[0]
            for i in range(OWN):
                fix[p, SIDE + 1, i] = jnp.where(lane == LANES - 1, turned[i + 1] if i + 1 < OWN else 0.0, turned[i])
            turned = [pltpu.roll(fix[p, SIDE, i], 1, 1) for i in range(OWN)]
            edge_out[1, p] = turned[OWN - 1]
            for i in range(OWN):
                fix[p, 0, i] = jnp.where(lane == 0, turned[i - 1] if i else 0.0, turned[i])
            for side in range(2):
                @pl.when(sides[side][0])
                def _():
                    edge(side, p).start()
    for p in range(2):
        arrived(4 + p)
        @pl.when(theres[p])
        def _():
            def step(x):
                lines = merged(first_of, x, outer[p], MIDDLE + p * SIDE + x)
                for i in range(OWN):
                    face1[p, x, i] = lines[i] + fix[p, x + 1, i]
            spread(4, step)
            face(1, p).start()
    for kind in range(6, KINDS):
        for only, count in ((across, EARLY_ACROSS), (paired, EARLY_PAIRED)):
            if kind - 6 >= count:
                send(kind, only)
    for p in range(2):
        @pl.when(theres[p])
        def _():
            face(1, 1 - p).wait_recv()
            @pl.loop(0, SIDE)
            def _(x):
                for i in range(OWN):
                    total = near1[p, x, i] + (fix[p, x, i] + fix[p, x + 2, i]) + sums(fix[p, x + 1, i])
                    change[p, 0, x, i] = total * inv[p, 0, x, i]

    def at(x, y, i):
        return pl.ds((x * SIDE + y) * (SIDE * OWN) + i, SIDE, stride=OWN)

    spots = {0: (0, 0), 1: (0, 1), SIDE - 2: (1, 1), SIDE - 1: (1, 0)}
    window = [i for i in range(OWN) if i < WIN or i >= OWN - WIN]

    @pl.loop(0, SIDE)
    def _(x):
        for y in range(SIDE):
            lines = aligned(second_of, x, y)
            for i in range(OWN):
                if i in window:
                    kept[x, y, window.index(i)] = lines[i]
                elif y in spots:
                    out[at(x, y, i), :] = lines[i] + change[spots[y][0], spots[y][1], x, i]
                else:
                    out[at(x, y, i), :] = lines[i]
    for p in range(2):
        for side, x, i, spot in ((0, 0, 0, 0), (1, SIDE - 1, OWN - 1, LANES - 1)):
            @pl.when(theres[p] & sides[side][0])
            def _():
                edge(1 - side, p).wait_recv()
                value = jnp.where(lane == spot, edge_in[side, p] * inv[p, 0, x, i], 0.0)
                change[p, 0, x, i] = change[p, 0, x, i] + value
    for x in range(SIDE):
        arrived(6 + x)
        for y in range(SIDE):
            a, b = windows(FINAL + x * SIDE + y)
            for j, i in enumerate(window):
                value = jnp.where(is_left[i], a[i], kept[x, y, j]) if i < WIN else jnp.where(
                    is_right[j - WIN], b[j - WIN], kept[x, y, j]
                )
                if y in spots:
                    value = value + change[spots[y][0], spots[y][1], x, i]
                out[at(x, y, i), :] = value
    for side in range(2):
        @pl.when(sides[side][0])
        def _():
            greeted(side).wait_send()
    for p in range(2):
        @pl.when(theres[p])
        def _():
            for b in range(2):
                face(b, p).wait_send()
            for side in range(2):
                @pl.when(sides[side][0])
                def _():
                    edge(side, p).wait_send()
    for kind in range(KINDS):
        for side in range(2):
            @pl.when(needed(kind, side))
            def _():
                sent(kind, side).wait_send()


def local(state, coef, counts):
    n, groups = lax.axis_size("curve"), lax.axis_size("grp")
    cells, cap = state.shape[1], state.shape[3]
    rows = cap // LANES
    plane = SIDE * SIDE * rows
    f32 = jnp.float32
    vmem, hbm, smem = (pl.BlockSpec(memory_space=m) for m in (pltpu.VMEM, pltpu.HBM, pltpu.SMEM))
    tile = (SIDE, LANES)
    shapes = [(cells * rows + 2 * plane, LANES), (cells * rows, LANES), (cells * rows + PAD, LANES)]
    shapes += [(cells * rows + 2 * PAD, LANES), (cells * rows + 2 * plane, LANES), (cells * rows + 2 * PAD, LANES)]
    shapes += [(2, UNITS, WIN) + tile] * 2
    shapes += [(2, SIDE, OWN) + tile] * 4
    shapes += [(2, 2, SIDE, OWN) + tile, (2, SIDE + 2, OWN) + tile, (2, 2, SIDE, OWN) + tile]
    shapes += [(SIDE, SIDE, 2 * WIN) + tile] + [(2, 2) + tile] * 2
    out = pl.pallas_call(
        functools.partial(exchange, n, groups, rows),
        out_shape=jax.ShapeDtypeStruct((cells * OWN, LANES), f32),
        in_specs=[smem, hbm, hbm],
        out_specs=vmem,
        scratch_shapes=[
            pltpu.VMEM((1, LANES), jnp.int32),
            pltpu.VMEM((n, 1, LANES), jnp.int32),
            pltpu.SMEM((n, 1, LANES), jnp.int32),
            pltpu.VMEM((2,) + tile, f32),
            pltpu.VMEM((2,) + tile, f32),
        ]
        + [pltpu.VMEM(shape, f32) for shape in shapes]
        + [pltpu.SemaphoreType.DMA((k,)) for k in (n, n, 2, 2, 2, 3, 2 * KINDS, 2 * KINDS, 4, 4, 4, 4)],
        compiler_params=pltpu.CompilerParams(
            collective_id=0, has_side_effects=True, vmem_limit_bytes=50 * 1024 * 1024
        ),
    )(
        counts, state.reshape(2, cells * rows, LANES), coef.reshape(cells * rows, LANES),
    )
    return out.reshape(cells, 1, AVG)


def solution(mesh):
    placed = (P(None, None, "grp", "curve"), P(None, "grp", "curve"), P("grp", "curve"))
    return jax.shard_map(
        local, mesh=mesh, in_specs=placed, out_specs=P(None, "grp", "curve"), check_vma=False
    )
```

```python
import functools

import jax
import jax.numpy as jnp
from jax import lax
from jax.experimental import pallas as pl
from jax.experimental.pallas import tpu as pltpu
from jax.sharding import PartitionSpec as P

AVG = 1024
HALF = 256
LANES = 128
SIDE = 8
WIN = HALF // LANES
OWN = AVG // LANES
PAD = 16
FIELD, FACTOR, MIDDLE, FINAL = 0, 2 * SIDE, 6 * SIDE, 8 * SIDE
UNITS = 16 * SIDE
KINDS = 8 + SIDE
MESH = pl.DeviceIdType.MESH
EARLY = 3


def exchange(
    n, groups, rows, counts, state, coef, out, mine, every, every_s, ends, met, raw0, raw1, raw2, inverse, first,
    second, put, got, face0, face1, near0, near1, inv, fix, change, kept, edge_out, edge_in, count_send, count_recv,
    end_send, end_recv, local_sem, load_sem, send_sem, recv_sem, face_send, face_recv, edge_send, edge_recv,
    via_end, via_end_send, via_end_recv, via, via_send, via_recv,
):
    plane_rows = SIDE * SIDE * rows
    cells_rows = SIDE * plane_rows
    rank, group = lax.axis_index("curve"), lax.axis_index("grp")
    has_left, has_right = rank > 0, rank < n - 1
    has_low, has_high = group > 0, group < groups - 1
    sides = (
        (has_left, {"curve": rank - 1}), (has_right, {"curve": rank + 1}),
        (has_low, {"grp": group - 1}), (has_high, {"grp": group + 1}),
    )
    theres = (has_low, has_high)
    raw = (raw0, raw1, raw2)
    front = (plane_rows, 0, 0)
    loads = {}
    for f, src in ((0, state.at[0]), (2, coef), (1, state.at[1])):
        loads[f] = pltpu.make_async_copy(src, raw[f].at[pl.ds(front[f], cells_rows)], load_sem.at[f])
        loads[f].start()
    barrier = pltpu.get_barrier_semaphore()
    for there, device in sides:
        @pl.when(there)
        def _():
            pl.semaphore_signal(barrier, inc=1, device_id=device, device_id_type=MESH)
    for off in range(2, n - 1):
        peer = lax.rem(rank + off, n)
        pl.semaphore_signal(barrier, inc=1, device_id={"curve": peer}, device_id_type=MESH)
    for there, peer in ((has_left, n - 1), (has_right, 0)):
        @pl.when(jnp.logical_not(there))
        def _():
            pl.semaphore_signal(barrier, inc=1, device_id={"curve": peer}, device_id_type=MESH)

    lane = lax.broadcasted_iota(jnp.int32, (SIDE, LANES), 1)
    level = lax.broadcasted_iota(jnp.int32, (SIDE, LANES), 0)
    held = jnp.clip(counts[0, 0], 2 * HALF, rows * LANES)
    mine[...] = jnp.full((1, LANES), held, jnp.int32)
    last = held - 1
    last_row, last_lane = lax.shift_right_logical(last, 7), last & (LANES - 1)
    tail_row = lax.shift_right_logical(held, 7) - WIN
    tail_part = held & (LANES - 1)
    tail_turn = (LANES - tail_part) & (LANES - 1)
    tail_stay = lane >= tail_part

    def raw_at(f, x, y, r):
        return pl.ds(front[f] + (x * SIDE + y) * (SIDE * rows) + r, SIDE, stride=rows)

    def field_of(x, y, r):
        return raw0[raw_at(0, x, y, r), :]

    def first_at(x, y, r):
        return pl.ds((((x + 1) * SIDE + y) * rows + r) * SIDE, SIDE)

    def flat_at(x, y, r):
        return pl.ds(PAD + ((x * SIDE + y) * rows + r) * SIDE, SIDE)

    def factor_of(x, y, r):
        return 1.0 / (raw2[raw_at(2, x, y, r), :] + 6.0)

    def pack(unit, get, x, y):
        for i in range(WIN):
            put[0, unit, i] = get(x, y, i)
        lines = [get(x, y, tail_row + i) for i in range(WIN + 1)]
        for i in range(WIN):
            put[1, unit, i] = pltpu.roll(jnp.where(tail_stay, lines[i], lines[i + 1]), tail_turn, 1)

    def message(kind):
        if kind < 2:
            return FIELD + kind * SIDE, SIDE
        if kind < 4:
            return FACTOR + (kind - 2) * SIDE, SIDE
        if kind < 6:
            return MIDDLE + (kind - 4) * SIDE, SIDE
        if kind < 8:
            return FACTOR + (kind - 4) * SIDE, SIDE
        return FINAL + (kind - 8) * SIDE, SIDE

    def sent(kind, side):
        start, count = message(kind)
        return pltpu.make_async_remote_copy(
            src_ref=put.at[side, pl.ds(start, count)], dst_ref=got.at[1 - side, pl.ds(start, count)],
            send_sem=send_sem.at[side * KINDS + kind], recv_sem=recv_sem.at[side * KINDS + kind],
            device_id=sides[side][1], device_id_type=MESH,
        )

    def needed(kind, side):
        return sides[side][0] & theres[kind % 2] if kind < 8 else sides[side][0]

    paired = lax.rem(rank, 2) == 1, lax.rem(rank, 2) == 0
    across = [jnp.logical_not(x) for x in paired]
    passes = paired[0] & (rank >= 2), paired[1] & (rank < n - 2)
    beyond = {"curve": rank - 2}, {"curve": rank + 2}
    steps = max(n // 2 - 1, 1)

    def routed(side, owner):
        return (owner if side == 0 else n - 1 - owner) // 2 * SIDE // steps

    def lent(c, side):
        start, count = message(8 + c)
        return pltpu.make_async_remote_copy(
            src_ref=put.at[side, pl.ds(start, count)], dst_ref=via.at[c],
            send_sem=send_sem.at[side * KINDS + 8 + c], recv_sem=via_recv.at[c],
            device_id=sides[1 - side][1], device_id_type=MESH,
        )

    def passed(c, side):
        start, count = message(8 + c)
        return pltpu.make_async_remote_copy(
            src_ref=via.at[c], dst_ref=got.at[1 - side, pl.ds(start, count)],
            send_sem=via_send.at[c], recv_sem=recv_sem.at[side * KINDS + 8 + c],
            device_id=beyond[side], device_id_type=MESH,
        )

    def lending(c, side):
        return sides[side][0] & across[side] & (c < routed(side, rank))

    def passing(c, side):
        return passes[side] & (c < routed(side, rank - 1 + 2 * side))

    def send(kind, only=(True, True)):
        for side in range(2):
            @pl.when(needed(kind, side) & only[side])
            def _():
                sent(kind, side).start()

    def arrived(kind):
        for side in range(2):
            @pl.when(needed(kind, side))
            def _():
                sent(kind, 1 - side).wait_recv()

    def spread(step, fn):
        @pl.loop(0, SIDE // step)
        def _(part):
            for at in range(step):
                fn(step * part + at)

    outer, inner = (0, SIDE - 1), (1, SIDE - 2)
    loads[0].wait()

    def step(x):
        for p in range(2):
            pack(FIELD + p * SIDE + x, field_of, x, outer[p])
    spread(4, step)
    loads[2].wait()
    loads[1].wait()
    for side, at, turn, outer_x, near_x in ((0, 0, 0, 1, 0), (1, last_row, LANES - last_lane, SIDE - 2, SIDE - 1)):
        packed = jnp.zeros((SIDE, LANES), jnp.float32)
        for p, (f, x) in enumerate(((0, outer_x), (0, near_x), (1, near_x), (2, near_x))):
            for y in range(SIDE):
                value = factor_of(x, y, at) if f == 2 else raw[f][raw_at(f, x, y, at), :]
                spot = p * SIDE + y
                value = pltpu.roll(value, (turn + spot) & (LANES - 1), 1)
                packed = jnp.where(lane == spot, value, packed)
        ends[side] = packed

    pl.semaphore_wait(barrier, n - 1 + has_low.astype(jnp.int32) + has_high.astype(jnp.int32))

    def greeted(side):
        return pltpu.make_async_remote_copy(
            src_ref=ends.at[side], dst_ref=met.at[1 - side], send_sem=end_send.at[side],
            recv_sem=end_recv.at[side], device_id=sides[side][1], device_id_type=MESH,
        )

    def greeted_via(side):
        return pltpu.make_async_remote_copy(
            src_ref=ends.at[side], dst_ref=via_end, send_sem=end_send.at[side],
            recv_sem=via_end_recv, device_id=sides[1 - side][1], device_id_type=MESH,
        )

    def greeted_on(side):
        return pltpu.make_async_remote_copy(
            src_ref=via_end, dst_ref=met.at[1 - side], send_sem=via_end_send,
            recv_sem=end_recv.at[side], device_id=beyond[side], device_id_type=MESH,
        )

    for side in range(2):
        @pl.when(sides[side][0] & across[side])
        def _():
            greeted_via(side).start()
    for side in range(2):
        @pl.when(sides[side][0] & paired[side])
        def _():
            greeted(side).start()
    tallies = []
    for off in range(1, n):
        tallies.append(
            pltpu.make_async_remote_copy(
                src_ref=mine, dst_ref=every.at[rank], send_sem=count_send.at[off],
                recv_sem=count_recv.at[off], device_id={"curve": lax.rem(rank + off, n)},
                device_id_type=MESH,
            )
        )
        tallies[-1].start()
    keep = pltpu.make_async_copy(mine, every.at[rank], local_sem.at[0])
    keep.start()
    for kind in range(2):
        send(kind)

    def step(x):
        for p in range(2):
            for k, y in enumerate((outer[p], inner[p])):
                pack(FACTOR + (2 * k + p) * SIDE + x, factor_of, x, y)
    spread(4, step)
    for kind in range(2, 4):
        send(kind)

    for side in range(2):
        @pl.when(passes[side])
        def _():
            greeted_via(side).wait_recv()
            greeted_on(side).start()
    for side in range(2):
        @pl.when(sides[side][0])
        def _():
            greeted(1 - side).wait_recv()
    shown = [ends[side] for side in range(2)]
    seen = [jnp.where(sides[side][0], met[side], 0.0) for side in range(2)]

    def sums(value):
        above = jnp.where(level < SIDE - 1, pltpu.roll(value, SIDE - 1, 0), 0.0)
        return above + jnp.where(level > 0, pltpu.roll(value, 1, 0), 0.0)

    def borders(get, store, ghosts, spot):
        def step(y):
            if True:
                turned = [pltpu.roll(get(SIDE - 1, y, r), 1, 1) for r in range(rows)]
                carry = pltpu.roll(ghosts[0], (LANES - spot - y) & (LANES - 1), 1)
                for r in range(rows):
                    store(-1, y, r, jnp.where(lane == 0, carry, turned[r]))
                    carry = turned[r]
                turned = [pltpu.roll(get(0, y, r), LANES - 1, 1) for r in range(rows)]
                ghost = pltpu.roll(ghosts[1], (last_lane + LANES - spot - y) & (LANES - 1), 1)
                for r in range(rows):
                    value = jnp.where(lane == LANES - 1, turned[r + 1], turned[r]) if r + 1 < rows else turned[r]
                    store(SIDE, y, r, jnp.where(lane + r * LANES == last, ghost, value))
        spread(4, step)

    def sweep(get, factor, store):
        @pl.loop(0, SIDE)
        def _(x):
            for r in range(rows):
                line = [get(x, y, r) for y in range(SIDE)]
                for y in range(SIDE):
                    total = (get(x - 1, y, r) + get(x + 1, y, r)) + (raw1[raw_at(1, x, y, r), :] + sums(line[y]))
                    if y > 0:
                        total = total + line[y - 1]
                    if y + 1 < SIDE:
                        total = total + line[y + 1]
                    store(x, y, r, total * factor(x, y, r))

    def store_field(x, y, r, value):
        raw0[raw_at(0, x, y, r), :] = value

    def first_of(x, y, r):
        return first[first_at(x, y, r), :]

    def store_first(x, y, r, value):
        first[first_at(x, y, r), :] = value

    def made_factor(x, y, r):
        value = factor_of(x, y, r)
        inverse[flat_at(x, y, r), :] = value
        return value

    def inverse_of(x, y, r):
        return inverse[flat_at(x, y, r), :]

    def second_of(x, y, r):
        return second[flat_at(x, y, r), :]

    def store_second(x, y, r, value):
        second[flat_at(x, y, r), :] = value

    borders(field_of, store_field, seen, SIDE)
    sweep(field_of, made_factor, store_first)

    def step(x):
        for p in range(2):
            pack(MIDDLE + p * SIDE + x, first_of, x, outer[p])
    spread(4, step)
    for kind in range(4, 8):
        send(kind)

    def moved(met_end, own_end):
        near = pltpu.roll(met_end, LANES - SIDE, 1)
        total = met_end + pltpu.roll(own_end, LANES - SIDE, 1) + sums(near)
        total = total + jnp.where(lane < SIDE - 1, pltpu.roll(near, LANES - 1, 1), 0.0)
        total = total + jnp.where(lane > 0, pltpu.roll(near, 1, 1), 0.0)
        total = total + pltpu.roll(met_end, LANES - 2 * SIDE, 1)
        return total * pltpu.roll(met_end, LANES - 3 * SIDE, 1)

    seen = [moved(seen[side], shown[side]) for side in range(2)]
    borders(first_of, store_first, seen, 0)
    sweep(first_of, inverse_of, store_second)

    def step(x):
        for y in range(SIDE):
            pack(FINAL + x * SIDE + y, second_of, x, y)
    spread(2, step)
    for c in range(SIDE):
        for side in range(2):
            @pl.when(lending(c, side))
            def _():
                lent(c, side).start()

    def release(early):
        for c in range(SIDE):
            for side in range(2):
                @pl.when(sides[side][0] & jnp.where(across[side], (c >= routed(side, rank)) & early, early == (c < EARLY)))
                def _():
                    sent(8 + c, side).start()
    release(True)
    keep.wait()
    for copy in tallies:
        copy.wait()
    keep = pltpu.make_async_copy(every, every_s, local_sem.at[1])
    keep.start()
    keep.wait()
    before = 0
    for r in range(n):
        before = before + jnp.where(r < rank, every_s[r, 0, 0], 0)
    drift_prev = jnp.clip(before - rank * AVG, -HALF, HALF)
    drift_next = jnp.clip(drift_prev + held - AVG, -HALF, HALF)
    base = lax.shift_right_arithmetic(-drift_prev, 7)
    part = (-drift_prev) & (LANES - 1)
    turn = (LANES - part) & (LANES - 1)
    stay = lane >= part
    shift = HALF - jnp.maximum(drift_prev, 0)
    left_part = shift & (LANES - 1)
    left_turn = (LANES - left_part) & (LANES - 1)
    left_pick = (lane >= left_part) & (shift < LANES)
    shift = -HALF - jnp.minimum(drift_next, 0)
    right_part = shift & (LANES - 1)
    right_turn = (LANES - right_part) & (LANES - 1)
    right_pick = (lane < right_part + jnp.where(shift == 0, LANES, 0)) & (shift >= -LANES)
    is_left = [lane + i * LANES < drift_prev for i in range(WIN)]
    is_right = [lane + i * LANES >= HALF + drift_next for i in range(WIN)]

    def aligned(get, x, y):
        lines = [get(x, y, base + i) for i in range(OWN + 1)]
        return [pltpu.roll(jnp.where(stay, lines[i], lines[i + 1]), turn, 1) for i in range(OWN)]

    def windows(unit):
        low, high = got[0, unit, 0], got[0, unit, 1]
        a = [pltpu.roll(jnp.where(left_pick, low, high), left_turn, 1), pltpu.roll(high, left_turn, 1)]
        low, high = got[1, unit, 0], got[1, unit, 1]
        b = [pltpu.roll(low, right_turn, 1), pltpu.roll(jnp.where(right_pick, high, low), right_turn, 1)]
        return a, b

    def merged(get, x, y, unit):
        lines = aligned(get, x, y)
        a, b = windows(unit)
        for i in range(WIN):
            lines[i] = jnp.where(is_left[i], a[i], lines[i])
            lines[OWN - WIN + i] = jnp.where(is_right[i], b[i], lines[OWN - WIN + i])
        return lines

    def face(b, p):
        src, dst = ((face0, near0), (face1, near1))[b]
        return pltpu.make_async_remote_copy(
            src_ref=src.at[p], dst_ref=dst.at[1 - p], send_sem=face_send.at[2 * b + p],
            recv_sem=face_recv.at[2 * b + p], device_id=sides[2 + p][1], device_id_type=MESH,
        )

    def edge(side, p):
        return pltpu.make_async_remote_copy(
            src_ref=edge_out.at[side, p], dst_ref=edge_in.at[1 - side, p], send_sem=edge_send.at[2 * side + p],
            recv_sem=edge_recv.at[2 * side + p], device_id=sides[side][1], device_id_type=MESH,
        )

    for p in range(2):
        arrived(p)
        @pl.when(theres[p])
        def _():
            def step(x):
                lines = merged(field_of, x, outer[p], FIELD + p * SIDE + x)
                for i in range(OWN):
                    face0[p, x, i] = lines[i]
            spread(4, step)
            face(0, p).start()
    for p in range(2):
        arrived(2 + p)
        @pl.when(theres[p])
        def _():
            def step(x):
                lines = merged(inverse_of, x, outer[p], FACTOR + p * SIDE + x)
                for i in range(OWN):
                    inv[p, x, i] = lines[i]
            spread(4, step)

        @pl.when(jnp.logical_not(theres[p]))
        def _():
            @pl.loop(0, SIDE)
            def _(x):
                for k in range(2):
                    for i in range(OWN):
                        change[p, k, x, i] = jnp.zeros((SIDE, LANES), jnp.float32)
    for p in range(2):
        @pl.when(theres[p])
        def _():
            face(0, 1 - p).wait_recv()
            @pl.loop(0, SIDE)
            def _(x):
                for i in range(OWN):
                    value = near0[p, x, i] * inv[p, x, i]
                    fix[p, x + 1, i] = value
            turned = [pltpu.roll(fix[p, 1, i], LANES - 1, 1) for i in range(OWN)]
            edge_out[0, p] = turned[0]
            for i in range(OWN):
                fix[p, SIDE + 1, i] = jnp.where(lane == LANES - 1, turned[i + 1] if i + 1 < OWN else 0.0, turned[i])
            turned = [pltpu.roll(fix[p, SIDE, i], 1, 1) for i in range(OWN)]
            edge_out[1, p] = turned[OWN - 1]
            for i in range(OWN):
                fix[p, 0, i] = jnp.where(lane == 0, turned[i - 1] if i else 0.0, turned[i])
            for side in range(2):
                @pl.when(sides[side][0])
                def _():
                    edge(side, p).start()
    for p in range(2):
        arrived(4 + p)
        @pl.when(theres[p])
        def _():
            def step(x):
                lines = merged(first_of, x, outer[p], MIDDLE + p * SIDE + x)
                for i in range(OWN):
                    face1[p, x, i] = lines[i] + fix[p, x + 1, i]
            spread(4, step)
            face(1, p).start()
    release(False)
    for p in range(2):
        @pl.when(theres[p])
        def _():
            face(1, 1 - p).wait_recv()
            @pl.loop(0, SIDE)
            def _(x):
                for i in range(OWN):
                    total = near1[p, x, i] + (fix[p, x, i] + fix[p, x + 2, i]) + sums(fix[p, x + 1, i])
                    change[p, 0, x, i] = total * inv[p, x, i]
    for p in range(2):
        arrived(6 + p)
        @pl.when(theres[p])
        def _():
            def step(x):
                lines = merged(inverse_of, x, inner[p], FACTOR + (2 + p) * SIDE + x)
                for i in range(OWN):
                    change[p, 1, x, i] = lines[i] * fix[p, x + 1, i]
            spread(4, step)
    for c in range(SIDE):
        for side in range(2):
            @pl.when(passing(c, side))
            def _():
                lent(c, side).wait_recv()
                passed(c, side).start()

    def at(x, y, i):
        return pl.ds((x * SIDE + y) * (SIDE * OWN) + i, SIDE, stride=OWN)

    spots = {0: (0, 0), 1: (0, 1), SIDE - 2: (1, 1), SIDE - 1: (1, 0)}
    window = [i for i in range(OWN) if i < WIN or i >= OWN - WIN]

    @pl.loop(0, SIDE)
    def _(x):
        for y in range(SIDE):
            lines = aligned(second_of, x, y)
            for i in range(OWN):
                if i in window:
                    kept[x, y, window.index(i)] = lines[i]
                elif y in spots:
                    out[at(x, y, i), :] = lines[i] + change[spots[y][0], spots[y][1], x, i]
                else:
                    out[at(x, y, i), :] = lines[i]
    def settle():
        for p in range(2):
            for side, x, i, spot in ((0, 0, 0, 0), (1, SIDE - 1, OWN - 1, LANES - 1)):
                @pl.when(theres[p] & sides[side][0])
                def _():
                    edge(1 - side, p).wait_recv()
                    value = jnp.where(lane == spot, edge_in[side, p] * inv[p, x, i], 0.0)
                    change[p, 0, x, i] = change[p, 0, x, i] + value

    for x in (1, 2, 3, 4, 5, 6, 0, 7):
        if x == 0:
            settle()
        arrived(8 + x)
        for y in range(SIDE):
            a, b = windows(FINAL + x * SIDE + y)
            for j, i in enumerate(window):
                value = jnp.where(is_left[i], a[i], kept[x, y, j]) if i < WIN else jnp.where(
                    is_right[j - WIN], b[j - WIN], kept[x, y, j]
                )
                if y in spots:
                    value = value + change[spots[y][0], spots[y][1], x, i]
                out[at(x, y, i), :] = value
    for side in range(2):
        @pl.when(passes[side])
        def _():
            greeted_on(side).wait_send()

        for c in range(SIDE):
            @pl.when(passing(c, side))
            def _():
                passed(c, side).wait_send()

        @pl.when(sides[side][0])
        def _():
            greeted(side).wait_send()
    for p in range(2):
        @pl.when(theres[p])
        def _():
            for b in range(2):
                face(b, p).wait_send()
            for side in range(2):
                @pl.when(sides[side][0])
                def _():
                    edge(side, p).wait_send()
    for kind in range(KINDS):
        for side in range(2):
            @pl.when(needed(kind, side))
            def _():
                sent(kind, side).wait_send()


def local(state, coef, counts):
    n, groups = lax.axis_size("curve"), lax.axis_size("grp")
    cells, cap = state.shape[1], state.shape[3]
    rows = cap // LANES
    plane = SIDE * SIDE * rows
    f32 = jnp.float32
    vmem, hbm, smem = (pl.BlockSpec(memory_space=m) for m in (pltpu.VMEM, pltpu.HBM, pltpu.SMEM))
    tile = (SIDE, LANES)
    shapes = [(cells * rows + 2 * plane, LANES), (cells * rows, LANES), (cells * rows + PAD, LANES)]
    shapes += [(cells * rows + 2 * PAD, LANES), (cells * rows + 2 * plane, LANES), (cells * rows + 2 * PAD, LANES)]
    shapes += [(2, UNITS, WIN) + tile] * 2
    shapes += [(2, SIDE, OWN) + tile] * 4
    shapes += [(2, SIDE, OWN) + tile, (2, SIDE + 2, OWN) + tile, (2, 2, SIDE, OWN) + tile]
    shapes += [(SIDE, SIDE, 2 * WIN) + tile] + [(2, 2) + tile] * 2
    out = pl.pallas_call(
        functools.partial(exchange, n, groups, rows),
        out_shape=jax.ShapeDtypeStruct((cells * OWN, LANES), f32),
        in_specs=[smem, hbm, hbm],
        out_specs=vmem,
        scratch_shapes=[
            pltpu.VMEM((1, LANES), jnp.int32),
            pltpu.VMEM((n, 1, LANES), jnp.int32),
            pltpu.SMEM((n, 1, LANES), jnp.int32),
            pltpu.VMEM((2,) + tile, f32),
            pltpu.VMEM((2,) + tile, f32),
        ]
        + [pltpu.VMEM(shape, f32) for shape in shapes]
        + [pltpu.SemaphoreType.DMA((k,)) for k in (n, n, 2, 2, 2, 3, 2 * KINDS, 2 * KINDS, 4, 4, 4, 4)]
        + [pltpu.VMEM(tile, f32)] + [pltpu.SemaphoreType.DMA] * 2
        + [pltpu.VMEM((SIDE, SIDE, WIN) + tile, f32)] + [pltpu.SemaphoreType.DMA((SIDE,))] * 2,
        compiler_params=pltpu.CompilerParams(
            collective_id=0, has_side_effects=True, vmem_limit_bytes=50 * 1024 * 1024
        ),
    )(
        counts, state.reshape(2, cells * rows, LANES), coef.reshape(cells * rows, LANES),
    )
    return out.reshape(cells, 1, AVG)


def solution(mesh):
    placed = (P(None, None, "grp", "curve"), P(None, "grp", "curve"), P("grp", "curve"))
    return jax.shard_map(
        local, mesh=mesh, in_specs=placed, out_specs=P(None, "grp", "curve"), check_vma=False
    )
```

```python
import functools

import jax
import jax.numpy as jnp
from jax import lax
from jax.experimental import pallas as pl
from jax.experimental.pallas import tpu as pltpu
from jax.sharding import PartitionSpec as P

AVG = 1024
HALF = 256
LANES = 128
SIDE = 8
WIN = HALF // LANES
OWN = AVG // LANES
PAD = 16
FIELD, FACTOR, MIDDLE, FINAL = 0, 2 * SIDE, 6 * SIDE, 8 * SIDE
UNITS = 16 * SIDE
KINDS = 8 + SIDE
MESH = pl.DeviceIdType.MESH
EARLY = 3


def exchange(
    n, groups, rows, counts, state, coef, out, mine, every, every_s, ends, met, raw0, raw1, raw2, inverse, first,
    second, put, got, face0, face1, near0, near1, inv, fix, change, kept, edge_out, edge_in, count_send, count_recv,
    end_send, end_recv, local_sem, load_sem, send_sem, recv_sem, face_send, face_recv, edge_send, edge_recv,
    via_end, via_end_send, via_end_recv, via, via_send, via_recv,
    rim,
):
    plane_rows = SIDE * SIDE * rows
    cells_rows = SIDE * plane_rows
    rank, group = lax.axis_index("curve"), lax.axis_index("grp")
    has_left, has_right = rank > 0, rank < n - 1
    has_low, has_high = group > 0, group < groups - 1
    sides = (
        (has_left, {"curve": rank - 1}), (has_right, {"curve": rank + 1}),
        (has_low, {"grp": group - 1}), (has_high, {"grp": group + 1}),
    )
    theres = (has_low, has_high)
    raw = (raw0, raw1, raw2)
    front = (plane_rows, 0, 0)
    band = SIDE * rows
    for p, y in enumerate((0, SIDE - 1)):
        for x in range(SIDE):
            pltpu.make_async_copy(
                state.at[0, pl.ds((x * SIDE + y) * band, band)], rim.at[pl.ds((p * SIDE + x) * band, band)], load_sem.at[3]
            ).start()
    sources = (state.at[0], state.at[1], coef)

    def load(f, x, count, sem):
        return pltpu.make_async_copy(
            sources[f].at[pl.ds(x * plane_rows, count * plane_rows)],
            raw[f].at[pl.ds(front[f] + x * plane_rows, count * plane_rows)], load_sem.at[sem],
        )

    for f, x, count in ((0, 0, 2), (0, SIDE - 2, 2), (1, 0, 1), (1, SIDE - 1, 1), (2, 0, 1), (2, SIDE - 1, 1)):
        load(f, x, count, 4).start()
    loads = {0: load(0, 2, SIDE - 4, 0), 2: load(2, 1, SIDE - 2, 2), 1: load(1, 1, SIDE - 2, 1)}
    for f in (2, 0, 1):
        loads[f].start()
    barrier = pltpu.get_barrier_semaphore()
    for there, device in sides:
        @pl.when(there)
        def _():
            pl.semaphore_signal(barrier, inc=1, device_id=device, device_id_type=MESH)
    for off in range(2, n - 1):
        peer = lax.rem(rank + off, n)
        pl.semaphore_signal(barrier, inc=1, device_id={"curve": peer}, device_id_type=MESH)
    for there, peer in ((has_left, n - 1), (has_right, 0)):
        @pl.when(jnp.logical_not(there))
        def _():
            pl.semaphore_signal(barrier, inc=1, device_id={"curve": peer}, device_id_type=MESH)

    lane = lax.broadcasted_iota(jnp.int32, (SIDE, LANES), 1)
    level = lax.broadcasted_iota(jnp.int32, (SIDE, LANES), 0)
    held = jnp.clip(counts[0, 0], 2 * HALF, rows * LANES)
    mine[...] = jnp.full((1, LANES), held, jnp.int32)
    last = held - 1
    last_row, last_lane = lax.shift_right_logical(last, 7), last & (LANES - 1)
    tail_row = lax.shift_right_logical(held, 7) - WIN
    tail_part = held & (LANES - 1)
    tail_turn = (LANES - tail_part) & (LANES - 1)
    tail_stay = lane >= tail_part

    def raw_at(f, x, y, r):
        return pl.ds(front[f] + (x * SIDE + y) * (SIDE * rows) + r, SIDE, stride=rows)

    def field_of(x, y, r):
        return raw0[raw_at(0, x, y, r), :]

    def first_at(x, y, r):
        return pl.ds((((x + 1) * SIDE + y) * rows + r) * SIDE, SIDE)

    def flat_at(x, y, r):
        return pl.ds(PAD + ((x * SIDE + y) * rows + r) * SIDE, SIDE)

    def factor_of(x, y, r):
        return 1.0 / (raw2[raw_at(2, x, y, r), :] + 6.0)

    def pack(unit, get, x, y):
        for i in range(WIN):
            put[0, unit, i] = get(x, y, i)
        lines = [get(x, y, tail_row + i) for i in range(WIN + 1)]
        for i in range(WIN):
            put[1, unit, i] = pltpu.roll(jnp.where(tail_stay, lines[i], lines[i + 1]), tail_turn, 1)

    def message(kind):
        if kind < 2:
            return FIELD + kind * SIDE, SIDE
        if kind < 4:
            return FACTOR + (kind - 2) * SIDE, SIDE
        if kind < 6:
            return MIDDLE + (kind - 4) * SIDE, SIDE
        if kind < 8:
            return FACTOR + (kind - 4) * SIDE, SIDE
        return FINAL + (kind - 8) * SIDE, SIDE

    def sent(kind, side):
        start, count = message(kind)
        return pltpu.make_async_remote_copy(
            src_ref=put.at[side, pl.ds(start, count)], dst_ref=got.at[1 - side, pl.ds(start, count)],
            send_sem=send_sem.at[3 * side + (kind % 2 if kind < 8 else 2)], recv_sem=recv_sem.at[side * KINDS + kind],
            device_id=sides[side][1], device_id_type=MESH,
        )

    def leaving(side, group):
        units = pl.ds(FINAL, SIDE * SIDE) if group == 2 else pl.ds(0, 4 * SIDE)
        return pltpu.make_async_remote_copy(
            src_ref=put.at[side, units], dst_ref=got.at[1 - side, units], send_sem=send_sem.at[3 * side + group],
            recv_sem=recv_sem.at[side * KINDS], device_id=sides[side][1], device_id_type=MESH,
        )

    def needed(kind, side):
        return sides[side][0] & theres[kind % 2] if kind < 8 else sides[side][0]

    paired = lax.rem(rank, 2) == 1, lax.rem(rank, 2) == 0
    across = [jnp.logical_not(x) for x in paired]
    passes = paired[0] & (rank >= 2), paired[1] & (rank < n - 2)
    beyond = {"curve": rank - 2}, {"curve": rank + 2}
    steps = max(n // 2 - 1, 1)

    def routed(side, owner):
        return (owner if side == 0 else n - 1 - owner) // 2 * (SIDE + 1) // steps

    def lent(c, side):
        start, count = message(8 + c)
        return pltpu.make_async_remote_copy(
            src_ref=put.at[side, pl.ds(start, count)], dst_ref=via.at[c],
            send_sem=send_sem.at[3 * side + 2], recv_sem=via_recv.at[c],
            device_id=sides[1 - side][1], device_id_type=MESH,
        )

    def passed(c, side):
        start, count = message(8 + c)
        return pltpu.make_async_remote_copy(
            src_ref=via.at[c], dst_ref=got.at[1 - side, pl.ds(start, count)],
            send_sem=via_send.at[c], recv_sem=recv_sem.at[side * KINDS + 8 + c],
            device_id=beyond[side], device_id_type=MESH,
        )

    def lending(c, side):
        return sides[side][0] & across[side] & (c < routed(side, rank))

    def passing(c, side):
        return passes[side] & (c < routed(side, rank - 1 + 2 * side))

    def send(kind, only=(True, True)):
        for side in range(2):
            @pl.when(needed(kind, side) & only[side])
            def _():
                sent(kind, side).start()

    def arrived(kind):
        for side in range(2):
            @pl.when(needed(kind, side))
            def _():
                sent(kind, 1 - side).wait_recv()

    def spread(step, fn):
        @pl.loop(0, SIDE // step)
        def _(part):
            for at in range(step):
                fn(step * part + at)

    outer, inner = (0, SIDE - 1), (1, SIDE - 2)
    pltpu.make_async_copy(
        state.at[0, pl.ds(0, 2 * SIDE * band)], rim.at[pl.ds(0, 2 * SIDE * band)], load_sem.at[3]
    ).wait()

    def rim_of(x, p, r):
        return rim[pl.ds((p * SIDE + x) * band + r, SIDE, stride=rows), :]

    def step(x):
        for p in range(2):
            pack(FIELD + p * SIDE + x, rim_of, x, p)
    spread(4, step)
    load(0, 0, SIDE, 4).wait()
    picks = [jnp.zeros((SIDE, LANES), jnp.int32) + last_row == r for r in range(rows)]

    def end_of(f, x, y, at):
        value = raw[f][raw_at(f, x, y, at), :]
        if at:
            for r in range(2 * HALF // LANES - 1, at):
                value = jnp.where(picks[r], raw[f][raw_at(f, x, y, r), :], value)
        return 1.0 / (value + 6.0) if f == 2 else value

    for side, at, turn, outer_x, near_x in ((0, 0, 0, 1, 0), (1, rows - 1, LANES - last_lane, SIDE - 2, SIDE - 1)):
        packed = jnp.zeros((SIDE, LANES), jnp.float32)
        for p, (f, x) in enumerate(((0, outer_x), (0, near_x), (1, near_x), (2, near_x))):
            for y in range(SIDE):
                value = end_of(f, x, y, at)
                spot = p * SIDE + y
                value = pltpu.roll(value, (turn + spot) & (LANES - 1), 1)
                packed = jnp.where(lane == spot, value, packed)
        ends[side] = packed

    pl.semaphore_wait(barrier, n - 1 + has_low.astype(jnp.int32) + has_high.astype(jnp.int32))

    def greeted(side):
        return pltpu.make_async_remote_copy(
            src_ref=ends.at[side], dst_ref=met.at[1 - side], send_sem=end_send.at[side],
            recv_sem=end_recv.at[side], device_id=sides[side][1], device_id_type=MESH,
        )

    def greeted_via(side):
        return pltpu.make_async_remote_copy(
            src_ref=ends.at[side], dst_ref=via_end, send_sem=end_send.at[side],
            recv_sem=via_end_recv, device_id=sides[1 - side][1], device_id_type=MESH,
        )

    def greeted_on(side):
        return pltpu.make_async_remote_copy(
            src_ref=via_end, dst_ref=met.at[1 - side], send_sem=via_end_send,
            recv_sem=end_recv.at[side], device_id=beyond[side], device_id_type=MESH,
        )

    for side in range(2):
        @pl.when(sides[side][0] & across[side])
        def _():
            greeted_via(side).start()
    for side in range(2):
        @pl.when(sides[side][0] & paired[side])
        def _():
            greeted(side).start()
    for off in range(1, n):
        pltpu.make_async_remote_copy(
            src_ref=mine, dst_ref=every.at[rank], send_sem=count_send, recv_sem=count_recv,
            device_id={"curve": lax.rem(rank + off, n)}, device_id_type=MESH,
        ).start()
    tallies = pltpu.make_async_remote_copy(
        src_ref=every.at[pl.ds(0, n - 1)], dst_ref=every.at[pl.ds(0, n - 1)], send_sem=count_send,
        recv_sem=count_recv, device_id={"curve": lax.rem(rank + 1, n)}, device_id_type=MESH,
    )
    keep = pltpu.make_async_copy(mine, every.at[rank], local_sem.at[0])
    keep.start()
    for kind in range(2):
        send(kind)
    for f in (2, 0, 1):
        loads[f].wait()

    def step(x):
        for p in range(2):
            for k, y in enumerate((outer[p], inner[p])):
                pack(FACTOR + (2 * k + p) * SIDE + x, factor_of, x, y)
    spread(4, step)
    for kind in range(2, 4):
        send(kind)

    for side in range(2):
        @pl.when(passes[side])
        def _():
            greeted_via(side).wait_recv()
            greeted_on(side).start()
    for side in range(2):
        @pl.when(sides[side][0])
        def _():
            greeted(1 - side).wait_recv()
    shown = [ends[side] for side in range(2)]
    seen = [jnp.where(sides[side][0], met[side], 0.0) for side in range(2)]

    def sums(value):
        above = jnp.where(level < SIDE - 1, pltpu.roll(value, SIDE - 1, 0), 0.0)
        return above + jnp.where(level > 0, pltpu.roll(value, 1, 0), 0.0)

    def borders(get, store, ghosts, spot):
        def step(y):
            if True:
                turned = [pltpu.roll(get(SIDE - 1, y, r), 1, 1) for r in range(rows)]
                carry = pltpu.roll(ghosts[0], (LANES - spot - y) & (LANES - 1), 1)
                for r in range(rows):
                    store(-1, y, r, jnp.where(lane == 0, carry, turned[r]))
                    carry = turned[r]
                turned = [pltpu.roll(get(0, y, r), LANES - 1, 1) for r in range(rows)]
                ghost = pltpu.roll(ghosts[1], (last_lane + LANES - spot - y) & (LANES - 1), 1)
                for r in range(rows):
                    value = jnp.where(lane == LANES - 1, turned[r + 1], turned[r]) if r + 1 < rows else turned[r]
                    store(SIDE, y, r, jnp.where(lane + r * LANES == last, ghost, value))
        spread(4, step)

    def sweep(get, factor, store):
        @pl.loop(0, SIDE)
        def _(x):
            for r in range(rows):
                line = [get(x, y, r) for y in range(SIDE)]
                for y in range(SIDE):
                    total = (get(x - 1, y, r) + get(x + 1, y, r)) + (raw1[raw_at(1, x, y, r), :] + sums(line[y]))
                    if y > 0:
                        total = total + line[y - 1]
                    if y + 1 < SIDE:
                        total = total + line[y + 1]
                    store(x, y, r, total * factor(x, y, r))

    def store_field(x, y, r, value):
        raw0[raw_at(0, x, y, r), :] = value

    def first_of(x, y, r):
        return first[first_at(x, y, r), :]

    def store_first(x, y, r, value):
        first[first_at(x, y, r), :] = value

    def made_factor(x, y, r):
        value = factor_of(x, y, r)
        inverse[flat_at(x, y, r), :] = value
        return value

    def inverse_of(x, y, r):
        return inverse[flat_at(x, y, r), :]

    def second_of(x, y, r):
        return second[flat_at(x, y, r), :]

    def store_second(x, y, r, value):
        second[flat_at(x, y, r), :] = value

    borders(field_of, store_field, seen, SIDE)
    sweep(field_of, made_factor, store_first)

    def step(x):
        for p in range(2):
            pack(MIDDLE + p * SIDE + x, first_of, x, outer[p])
    spread(4, step)
    for kind in range(4, 8):
        send(kind)

    def moved(met_end, own_end):
        near = pltpu.roll(met_end, LANES - SIDE, 1)
        total = met_end + pltpu.roll(own_end, LANES - SIDE, 1) + sums(near)
        total = total + jnp.where(lane < SIDE - 1, pltpu.roll(near, LANES - 1, 1), 0.0)
        total = total + jnp.where(lane > 0, pltpu.roll(near, 1, 1), 0.0)
        total = total + pltpu.roll(met_end, LANES - 2 * SIDE, 1)
        return total * pltpu.roll(met_end, LANES - 3 * SIDE, 1)

    seen = [moved(seen[side], shown[side]) for side in range(2)]
    borders(first_of, store_first, seen, 0)
    sweep(first_of, inverse_of, store_second)

    def step(x):
        for y in range(SIDE):
            pack(FINAL + x * SIDE + y, second_of, x, y)
    spread(2, step)
    for c in range(SIDE):
        for side in range(2):
            @pl.when(lending(c, side))
            def _():
                lent(c, side).start()

    soon = jnp.where((rank == 1) | (rank == n - 2), SIDE, EARLY)

    def release(early):
        for c in range(SIDE):
            for side in range(2):
                @pl.when(sides[side][0] & jnp.where(across[side], (c >= routed(side, rank)) & early, early == (c < soon)))
                def _():
                    sent(8 + c, side).start()
    release(True)
    keep.wait()
    tallies.wait()
    keep = pltpu.make_async_copy(every, every_s, local_sem.at[1])
    keep.start()
    keep.wait()
    before = 0
    for r in range(n):
        before = before + jnp.where(r < rank, every_s[r, 0, 0], 0)
    drift_prev = jnp.clip(before - rank * AVG, -HALF, HALF)
    drift_next = jnp.clip(drift_prev + held - AVG, -HALF, HALF)
    base = lax.shift_right_arithmetic(-drift_prev, 7)
    part = (-drift_prev) & (LANES - 1)
    turn = (LANES - part) & (LANES - 1)
    stay = lane >= part
    shift = HALF - jnp.maximum(drift_prev, 0)
    left_part = shift & (LANES - 1)
    left_turn = (LANES - left_part) & (LANES - 1)
    left_pick = (lane >= left_part) & (shift < LANES)
    shift = -HALF - jnp.minimum(drift_next, 0)
    right_part = shift & (LANES - 1)
    right_turn = (LANES - right_part) & (LANES - 1)
    right_pick = (lane < right_part + jnp.where(shift == 0, LANES, 0)) & (shift >= -LANES)
    is_left = [lane + i * LANES < drift_prev for i in range(WIN)]
    is_right = [lane + i * LANES >= HALF + drift_next for i in range(WIN)]

    def aligned(get, x, y):
        lines = [get(x, y, base + i) for i in range(OWN + 1)]
        return [pltpu.roll(jnp.where(stay, lines[i], lines[i + 1]), turn, 1) for i in range(OWN)]

    def windows(unit):
        low, high = got[0, unit, 0], got[0, unit, 1]
        a = [pltpu.roll(jnp.where(left_pick, low, high), left_turn, 1), pltpu.roll(high, left_turn, 1)]
        low, high = got[1, unit, 0], got[1, unit, 1]
        b = [pltpu.roll(low, right_turn, 1), pltpu.roll(jnp.where(right_pick, high, low), right_turn, 1)]
        return a, b

    def merged(get, x, y, unit):
        lines = aligned(get, x, y)
        a, b = windows(unit)
        for i in range(WIN):
            lines[i] = jnp.where(is_left[i], a[i], lines[i])
            lines[OWN - WIN + i] = jnp.where(is_right[i], b[i], lines[OWN - WIN + i])
        return lines

    def face(b, p):
        src, dst = ((face0, near0), (face1, near1))[b]
        return pltpu.make_async_remote_copy(
            src_ref=src.at[p], dst_ref=dst.at[1 - p], send_sem=face_send.at[2 * b + p],
            recv_sem=face_recv.at[2 * b + p], device_id=sides[2 + p][1], device_id_type=MESH,
        )

    def edge(side, p):
        return pltpu.make_async_remote_copy(
            src_ref=edge_out.at[side, p], dst_ref=edge_in.at[1 - side, p], send_sem=edge_send.at[2 * side + p],
            recv_sem=edge_recv.at[2 * side + p], device_id=sides[side][1], device_id_type=MESH,
        )

    for p in range(2):
        arrived(p)
        @pl.when(theres[p])
        def _():
            def step(x):
                lines = merged(field_of, x, outer[p], FIELD + p * SIDE + x)
                for i in range(OWN):
                    face0[p, x, i] = lines[i]
            spread(4, step)
            face(0, p).start()
    for p in range(2):
        arrived(2 + p)
        @pl.when(theres[p])
        def _():
            def step(x):
                lines = merged(inverse_of, x, outer[p], FACTOR + p * SIDE + x)
                for i in range(OWN):
                    inv[p, x, i] = lines[i]
            spread(4, step)

        @pl.when(jnp.logical_not(theres[p]))
        def _():
            @pl.loop(0, SIDE)
            def _(x):
                for k in range(2):
                    for i in range(OWN):
                        change[p, k, x, i] = jnp.zeros((SIDE, LANES), jnp.float32)
    for p in range(2):
        @pl.when(theres[p])
        def _():
            face(0, 1 - p).wait_recv()
            @pl.loop(0, SIDE)
            def _(x):
                for i in range(OWN):
                    value = near0[p, x, i] * inv[p, x, i]
                    fix[p, x + 1, i] = value
            turned = [pltpu.roll(fix[p, 1, i], LANES - 1, 1) for i in range(OWN)]
            edge_out[0, p] = turned[0]
            for i in range(OWN):
                fix[p, SIDE + 1, i] = jnp.where(lane == LANES - 1, turned[i + 1] if i + 1 < OWN else 0.0, turned[i])
            turned = [pltpu.roll(fix[p, SIDE, i], 1, 1) for i in range(OWN)]
            edge_out[1, p] = turned[OWN - 1]
            for i in range(OWN):
                fix[p, 0, i] = jnp.where(lane == 0, turned[i - 1] if i else 0.0, turned[i])
            for side in range(2):
                @pl.when(sides[side][0])
                def _():
                    edge(side, p).start()
    for p in range(2):
        arrived(4 + p)
        @pl.when(theres[p])
        def _():
            def step(x):
                lines = merged(first_of, x, outer[p], MIDDLE + p * SIDE + x)
                for i in range(OWN):
                    face1[p, x, i] = lines[i] + fix[p, x + 1, i]
            spread(4, step)
            face(1, p).start()
    release(False)
    for p in range(2):
        @pl.when(theres[p])
        def _():
            face(1, 1 - p).wait_recv()
            @pl.loop(0, SIDE)
            def _(x):
                for i in range(OWN):
                    total = near1[p, x, i] + (fix[p, x, i] + fix[p, x + 2, i]) + sums(fix[p, x + 1, i])
                    change[p, 0, x, i] = total * inv[p, x, i]
    for p in range(2):
        arrived(6 + p)
        @pl.when(theres[p])
        def _():
            def step(x):
                lines = merged(inverse_of, x, inner[p], FACTOR + (2 + p) * SIDE + x)
                for i in range(OWN):
                    change[p, 1, x, i] = lines[i] * fix[p, x + 1, i]
            spread(4, step)
    for c in range(SIDE):
        for side in range(2):
            @pl.when(passing(c, side))
            def _():
                lent(c, side).wait_recv()
                passed(c, side).start()

    def at(x, y, i):
        return pl.ds((x * SIDE + y) * (SIDE * OWN) + i, SIDE, stride=OWN)

    spots = {0: (0, 0), 1: (0, 1), SIDE - 2: (1, 1), SIDE - 1: (1, 0)}
    window = [i for i in range(OWN) if i < WIN or i >= OWN - WIN]

    @pl.loop(0, SIDE)
    def _(x):
        for y in range(SIDE):
            lines = aligned(second_of, x, y)
            for i in range(OWN):
                if i in window:
                    kept[x, y, window.index(i)] = lines[i]
                elif y in spots:
                    out[at(x, y, i), :] = lines[i] + change[spots[y][0], spots[y][1], x, i]
                else:
                    out[at(x, y, i), :] = lines[i]
    def settle():
        for p in range(2):
            for side, x, i, spot in ((0, 0, 0, 0), (1, SIDE - 1, OWN - 1, LANES - 1)):
                @pl.when(theres[p] & sides[side][0])
                def _():
                    edge(1 - side, p).wait_recv()
                    value = jnp.where(lane == spot, edge_in[side, p] * inv[p, x, i], 0.0)
                    change[p, 0, x, i] = change[p, 0, x, i] + value

    for x in (1, 2, 3, 4, 5, 6, 0, 7):
        if x == 0:
            settle()
        arrived(8 + x)
        for y in range(SIDE):
            a, b = windows(FINAL + x * SIDE + y)
            for j, i in enumerate(window):
                value = jnp.where(is_left[i], a[i], kept[x, y, j]) if i < WIN else jnp.where(
                    is_right[j - WIN], b[j - WIN], kept[x, y, j]
                )
                if y in spots:
                    value = value + change[spots[y][0], spots[y][1], x, i]
                out[at(x, y, i), :] = value
    for side in range(2):
        @pl.when(passes[side])
        def _():
            greeted_on(side).wait_send()

        for c in range(SIDE):
            @pl.when(passing(c, side))
            def _():
                passed(c, side).wait_send()

        @pl.when(sides[side][0])
        def _():
            greeted(side).wait_send()
    for p in range(2):
        @pl.when(theres[p])
        def _():
            for b in range(2):
                face(b, p).wait_send()
            for side in range(2):
                @pl.when(sides[side][0])
                def _():
                    edge(side, p).wait_send()
    for side in range(2):
        for group, there in enumerate((has_low, has_high, True)):
            @pl.when(sides[side][0] & there)
            def _():
                leaving(side, group).wait_send()


def local(state, coef, counts):
    n, groups = lax.axis_size("curve"), lax.axis_size("grp")
    cells, cap = state.shape[1], state.shape[3]
    rows = cap // LANES
    plane = SIDE * SIDE * rows
    f32 = jnp.float32
    vmem, hbm, smem = (pl.BlockSpec(memory_space=m) for m in (pltpu.VMEM, pltpu.HBM, pltpu.SMEM))
    tile = (SIDE, LANES)
    shapes = [(cells * rows + 2 * plane, LANES), (cells * rows, LANES), (cells * rows + PAD, LANES)]
    shapes += [(cells * rows + 2 * PAD, LANES), (cells * rows + 2 * plane, LANES), (cells * rows + 2 * PAD, LANES)]
    shapes += [(2, UNITS, WIN) + tile] * 2
    shapes += [(2, SIDE, OWN) + tile] * 4
    shapes += [(2, SIDE, OWN) + tile, (2, SIDE + 2, OWN) + tile, (2, 2, SIDE, OWN) + tile]
    shapes += [(SIDE, SIDE, 2 * WIN) + tile] + [(2, 2) + tile] * 2
    out = pl.pallas_call(
        functools.partial(exchange, n, groups, rows),
        out_shape=jax.ShapeDtypeStruct((cells * OWN, LANES), f32),
        in_specs=[smem, hbm, hbm],
        out_specs=vmem,
        scratch_shapes=[
            pltpu.VMEM((1, LANES), jnp.int32),
            pltpu.VMEM((n, 1, LANES), jnp.int32),
            pltpu.SMEM((n, 1, LANES), jnp.int32),
            pltpu.VMEM((2,) + tile, f32),
            pltpu.VMEM((2,) + tile, f32),
        ]
        + [pltpu.VMEM(shape, f32) for shape in shapes]
        + [pltpu.SemaphoreType.DMA] * 2
        + [pltpu.SemaphoreType.DMA((k,)) for k in (2, 2, 2, 5, 6, 2 * KINDS, 4, 4, 4, 4)]
        + [pltpu.VMEM(tile, f32)] + [pltpu.SemaphoreType.DMA] * 2
        + [pltpu.VMEM((SIDE, SIDE, WIN) + tile, f32)] + [pltpu.SemaphoreType.DMA((SIDE,))] * 2
        + [pltpu.VMEM((2 * SIDE * SIDE * rows + PAD, LANES), f32)],
        compiler_params=pltpu.CompilerParams(
            collective_id=0, has_side_effects=True, vmem_limit_bytes=50 * 1024 * 1024
        ),
    )(
        counts, state.reshape(2, cells * rows, LANES), coef.reshape(cells * rows, LANES),
    )
    return out.reshape(cells, 1, AVG)


def solution(mesh):
    placed = (P(None, None, "grp", "curve"), P(None, "grp", "curve"), P("grp", "curve"))
    return jax.shard_map(
        local, mesh=mesh, in_specs=placed, out_specs=P(None, "grp", "curve"), check_vma=False
    )
```

```python
import functools

import jax
import jax.numpy as jnp
from jax import lax
from jax.experimental import pallas as pl
from jax.experimental.pallas import tpu as pltpu
from jax.sharding import PartitionSpec as P

AVG = 1024
HALF = 256
LANES = 128
SIDE = 8
WIN = HALF // LANES
OWN = AVG // LANES
PAD = 16
FIELD, FACTOR, MIDDLE, FINAL = 0, 2 * SIDE, 6 * SIDE, 8 * SIDE
UNITS = 16 * SIDE
KINDS = 8 + SIDE
MESH = pl.DeviceIdType.MESH
EARLY = 3


def exchange(
    n, groups, rows, counts, state, coef, out, mine, every, every_s, ends, met, raw0, raw1, raw2, inverse, first,
    second, put, got, face0, face1, near0, near1, inv, fix, change, kept, edge_out, edge_in, count_send, count_recv,
    end_send, end_recv, local_sem, load_sem, send_sem, recv_sem, face_send, face_recv, edge_send, edge_recv,
    via_end, via_end_send, via_end_recv, via, via_send, via_recv,
    rim,
):
    plane_rows = SIDE * SIDE * rows
    cells_rows = SIDE * plane_rows
    rank, group = lax.axis_index("curve"), lax.axis_index("grp")
    has_left, has_right = rank > 0, rank < n - 1
    has_low, has_high = group > 0, group < groups - 1
    sides = (
        (has_left, {"curve": rank - 1}), (has_right, {"curve": rank + 1}),
        (has_low, {"grp": group - 1}), (has_high, {"grp": group + 1}),
    )
    theres = (has_low, has_high)
    raw = (raw0, raw1, raw2)
    front = (plane_rows, 0, 0)
    band = SIDE * rows
    for p, y in enumerate((0, SIDE - 1)):
        for x in range(SIDE):
            pltpu.make_async_copy(
                state.at[0, pl.ds((x * SIDE + y) * band, band)], rim.at[pl.ds((p * SIDE + x) * band, band)], load_sem.at[3]
            ).start()
    sources = (state.at[0], state.at[1], coef)

    def load(f, x, count, sem):
        return pltpu.make_async_copy(
            sources[f].at[pl.ds(x * plane_rows, count * plane_rows)],
            raw[f].at[pl.ds(front[f] + x * plane_rows, count * plane_rows)], load_sem.at[sem],
        )

    for f, x, count in ((0, 0, 2), (0, SIDE - 2, 2), (1, 0, 1), (1, SIDE - 1, 1), (2, 0, 1), (2, SIDE - 1, 1)):
        load(f, x, count, 4).start()
    loads = {0: load(0, 2, SIDE - 4, 0), 2: load(2, 1, SIDE - 2, 2), 1: load(1, 1, SIDE - 2, 1)}
    for f in (2, 0, 1):
        loads[f].start()
    barrier = pltpu.get_barrier_semaphore()
    for there, device in sides[2:]:
        @pl.when(there)
        def _():
            pl.semaphore_signal(barrier, inc=1, device_id=device, device_id_type=MESH)
    half = n // 2
    lower = rank < half
    base_rank = jnp.where(lower, 0, half)
    place = rank - base_rank
    mates = [base_rank + lax.rem(place + off, half) for off in range(1, half)]
    asked = half - 1
    for peer in mates:
        pl.semaphore_signal(barrier, inc=1, device_id={"curve": peer}, device_id_type=MESH)
    for there, device in sides[2:]:
        asked = asked + there.astype(jnp.int32)
    for off in (-2, -1, 1, 2):
        peer = rank + off
        there = (peer >= 0) & (peer < n) & (lower != (peer < half))
        asked = asked + there.astype(jnp.int32)
        @pl.when(there)
        def _():
            pl.semaphore_signal(barrier, inc=1, device_id={"curve": peer}, device_id_type=MESH)

    lane = lax.broadcasted_iota(jnp.int32, (SIDE, LANES), 1)
    level = lax.broadcasted_iota(jnp.int32, (SIDE, LANES), 0)
    held = jnp.clip(counts[0, 0], 2 * HALF, rows * LANES)
    mine[...] = jnp.full((1, LANES), held, jnp.int32)
    last = held - 1
    last_row, last_lane = lax.shift_right_logical(last, 7), last & (LANES - 1)
    tail_row = lax.shift_right_logical(held, 7) - WIN
    tail_part = held & (LANES - 1)
    tail_turn = (LANES - tail_part) & (LANES - 1)
    tail_stay = lane >= tail_part

    def raw_at(f, x, y, r):
        return pl.ds(front[f] + (x * SIDE + y) * (SIDE * rows) + r, SIDE, stride=rows)

    def field_of(x, y, r):
        return raw0[raw_at(0, x, y, r), :]

    def first_at(x, y, r):
        return pl.ds((((x + 1) * SIDE + y) * rows + r) * SIDE, SIDE)

    def flat_at(x, y, r):
        return pl.ds(PAD + ((x * SIDE + y) * rows + r) * SIDE, SIDE)

    def factor_of(x, y, r):
        return 1.0 / (raw2[raw_at(2, x, y, r), :] + 6.0)

    def pack(unit, get, x, y):
        for i in range(WIN):
            put[0, unit, i] = get(x, y, i)
        lines = [get(x, y, tail_row + i) for i in range(WIN + 1)]
        for i in range(WIN):
            put[1, unit, i] = pltpu.roll(jnp.where(tail_stay, lines[i], lines[i + 1]), tail_turn, 1)

    def message(kind):
        if kind < 2:
            return FIELD + kind * SIDE, SIDE
        if kind < 4:
            return FACTOR + (kind - 2) * SIDE, SIDE
        if kind < 6:
            return MIDDLE + (kind - 4) * SIDE, SIDE
        if kind < 8:
            return FACTOR + (kind - 4) * SIDE, SIDE
        return FINAL + (kind - 8) * SIDE, SIDE

    def sent(kind, side):
        start, count = message(kind)
        return pltpu.make_async_remote_copy(
            src_ref=put.at[side, pl.ds(start, count)], dst_ref=got.at[1 - side, pl.ds(start, count)],
            send_sem=send_sem.at[3 * side + (kind % 2 if kind < 8 else 2)], recv_sem=recv_sem.at[side * KINDS + kind],
            device_id=sides[side][1], device_id_type=MESH,
        )

    def leaving(side, group):
        units = pl.ds(FINAL, SIDE * SIDE) if group == 2 else pl.ds(0, 4 * SIDE)
        return pltpu.make_async_remote_copy(
            src_ref=put.at[side, units], dst_ref=got.at[1 - side, units], send_sem=send_sem.at[3 * side + group],
            recv_sem=recv_sem.at[side * KINDS], device_id=sides[side][1], device_id_type=MESH,
        )

    def needed(kind, side):
        return sides[side][0] & theres[kind % 2] if kind < 8 else sides[side][0]

    paired = lax.rem(rank, 2) == 1, lax.rem(rank, 2) == 0
    across = [jnp.logical_not(x) for x in paired]
    passes = paired[0] & (rank >= 2), paired[1] & (rank < n - 2)
    beyond = {"curve": rank - 2}, {"curve": rank + 2}
    steps = max(n // 2 - 1, 1)

    def routed(side, owner):
        return (owner if side == 0 else n - 1 - owner) // 2 * (SIDE + 1) // steps

    def lent(c, side):
        start, count = message(8 + c)
        return pltpu.make_async_remote_copy(
            src_ref=put.at[side, pl.ds(start, count)], dst_ref=via.at[c],
            send_sem=send_sem.at[3 * side + 2], recv_sem=via_recv.at[c],
            device_id=sides[1 - side][1], device_id_type=MESH,
        )

    def passed(c, side):
        start, count = message(8 + c)
        return pltpu.make_async_remote_copy(
            src_ref=via.at[c], dst_ref=got.at[1 - side, pl.ds(start, count)],
            send_sem=via_send.at[c], recv_sem=recv_sem.at[side * KINDS + 8 + c],
            device_id=beyond[side], device_id_type=MESH,
        )

    def lending(c, side):
        return sides[side][0] & across[side] & (c < routed(side, rank))

    def passing(c, side):
        return passes[side] & (c < routed(side, rank - 1 + 2 * side))

    def send(kind, only=(True, True)):
        for side in range(2):
            @pl.when(needed(kind, side) & only[side])
            def _():
                sent(kind, side).start()

    def arrived(kind):
        for side in range(2):
            @pl.when(needed(kind, side))
            def _():
                sent(kind, 1 - side).wait_recv()

    def spread(step, fn):
        @pl.loop(0, SIDE // step)
        def _(part):
            for at in range(step):
                fn(step * part + at)

    outer, inner = (0, SIDE - 1), (1, SIDE - 2)
    pltpu.make_async_copy(
        state.at[0, pl.ds(0, 2 * SIDE * band)], rim.at[pl.ds(0, 2 * SIDE * band)], load_sem.at[3]
    ).wait()

    def rim_of(x, p, r):
        return rim[pl.ds((p * SIDE + x) * band + r, SIDE, stride=rows), :]

    def step(x):
        for p in range(2):
            pack(FIELD + p * SIDE + x, rim_of, x, p)
    spread(4, step)
    load(0, 0, SIDE, 4).wait()
    picks = [jnp.zeros((SIDE, LANES), jnp.int32) + last_row == r for r in range(rows)]

    def end_of(f, x, y, at):
        value = raw[f][raw_at(f, x, y, at), :]
        if at:
            for r in range(2 * HALF // LANES - 1, at):
                value = jnp.where(picks[r], raw[f][raw_at(f, x, y, r), :], value)
        return 1.0 / (value + 6.0) if f == 2 else value

    for side, at, turn, outer_x, near_x in ((0, 0, 0, 1, 0), (1, rows - 1, LANES - last_lane, SIDE - 2, SIDE - 1)):
        packed = jnp.zeros((SIDE, LANES), jnp.float32)
        for p, (f, x) in enumerate(((0, outer_x), (0, near_x), (1, near_x), (2, near_x))):
            for y in range(SIDE):
                value = end_of(f, x, y, at)
                spot = p * SIDE + y
                value = pltpu.roll(value, (turn + spot) & (LANES - 1), 1)
                packed = jnp.where(lane == spot, value, packed)
        ends[side] = packed

    pl.semaphore_wait(barrier, asked)

    def greeted(side):
        return pltpu.make_async_remote_copy(
            src_ref=ends.at[side], dst_ref=met.at[1 - side], send_sem=end_send.at[side],
            recv_sem=end_recv.at[side], device_id=sides[side][1], device_id_type=MESH,
        )

    def greeted_via(side):
        return pltpu.make_async_remote_copy(
            src_ref=ends.at[side], dst_ref=via_end, send_sem=end_send.at[side],
            recv_sem=via_end_recv, device_id=sides[1 - side][1], device_id_type=MESH,
        )

    def greeted_on(side):
        return pltpu.make_async_remote_copy(
            src_ref=via_end, dst_ref=met.at[1 - side], send_sem=via_end_send,
            recv_sem=end_recv.at[side], device_id=beyond[side], device_id_type=MESH,
        )

    for side in range(2):
        @pl.when(sides[side][0] & across[side])
        def _():
            greeted_via(side).start()
    for side in range(2):
        @pl.when(sides[side][0] & paired[side])
        def _():
            greeted(side).start()
    for peer in mates:
        pltpu.make_async_remote_copy(
            src_ref=mine, dst_ref=every.at[place], send_sem=count_send, recv_sem=count_recv,
            device_id={"curve": peer}, device_id_type=MESH,
        ).start()
    tallies = pltpu.make_async_remote_copy(
        src_ref=every.at[pl.ds(0, half - 1)], dst_ref=every.at[pl.ds(0, half - 1)], send_sem=count_send,
        recv_sem=count_recv, device_id={"curve": mates[0]}, device_id_type=MESH,
    )
    keep = pltpu.make_async_copy(mine, every.at[place], local_sem.at[0])
    keep.start()
    for kind in range(2):
        send(kind)
    for f in (2, 0, 1):
        loads[f].wait()

    def step(x):
        for p in range(2):
            for k, y in enumerate((outer[p], inner[p])):
                pack(FACTOR + (2 * k + p) * SIDE + x, factor_of, x, y)
    spread(4, step)
    for kind in range(2, 4):
        send(kind)

    for side in range(2):
        @pl.when(passes[side])
        def _():
            greeted_via(side).wait_recv()
            greeted_on(side).start()
    for side in range(2):
        @pl.when(sides[side][0])
        def _():
            greeted(1 - side).wait_recv()
    shown = [ends[side] for side in range(2)]
    seen = [jnp.where(sides[side][0], met[side], 0.0) for side in range(2)]

    def sums(value):
        above = jnp.where(level < SIDE - 1, pltpu.roll(value, SIDE - 1, 0), 0.0)
        return above + jnp.where(level > 0, pltpu.roll(value, 1, 0), 0.0)

    def borders(get, store, ghosts, spot):
        def step(y):
            if True:
                turned = [pltpu.roll(get(SIDE - 1, y, r), 1, 1) for r in range(rows)]
                carry = pltpu.roll(ghosts[0], (LANES - spot - y) & (LANES - 1), 1)
                for r in range(rows):
                    store(-1, y, r, jnp.where(lane == 0, carry, turned[r]))
                    carry = turned[r]
                turned = [pltpu.roll(get(0, y, r), LANES - 1, 1) for r in range(rows)]
                ghost = pltpu.roll(ghosts[1], (last_lane + LANES - spot - y) & (LANES - 1), 1)
                for r in range(rows):
                    value = jnp.where(lane == LANES - 1, turned[r + 1], turned[r]) if r + 1 < rows else turned[r]
                    store(SIDE, y, r, jnp.where(lane + r * LANES == last, ghost, value))
        spread(4, step)

    def sweep(get, factor, store):
        @pl.loop(0, SIDE)
        def _(x):
            for r in range(rows):
                line = [get(x, y, r) for y in range(SIDE)]
                for y in range(SIDE):
                    total = (get(x - 1, y, r) + get(x + 1, y, r)) + (raw1[raw_at(1, x, y, r), :] + sums(line[y]))
                    if y > 0:
                        total = total + line[y - 1]
                    if y + 1 < SIDE:
                        total = total + line[y + 1]
                    store(x, y, r, total * factor(x, y, r))

    def store_field(x, y, r, value):
        raw0[raw_at(0, x, y, r), :] = value

    def first_of(x, y, r):
        return first[first_at(x, y, r), :]

    def store_first(x, y, r, value):
        first[first_at(x, y, r), :] = value

    def made_factor(x, y, r):
        value = factor_of(x, y, r)
        inverse[flat_at(x, y, r), :] = value
        return value

    def inverse_of(x, y, r):
        return inverse[flat_at(x, y, r), :]

    def second_of(x, y, r):
        return second[flat_at(x, y, r), :]

    def store_second(x, y, r, value):
        second[flat_at(x, y, r), :] = value

    borders(field_of, store_field, seen, SIDE)
    sweep(field_of, made_factor, store_first)

    def step(x):
        for p in range(2):
            pack(MIDDLE + p * SIDE + x, first_of, x, outer[p])
    spread(4, step)
    for kind in range(4, 8):
        send(kind)

    def moved(met_end, own_end):
        near = pltpu.roll(met_end, LANES - SIDE, 1)
        total = met_end + pltpu.roll(own_end, LANES - SIDE, 1) + sums(near)
        total = total + jnp.where(lane < SIDE - 1, pltpu.roll(near, LANES - 1, 1), 0.0)
        total = total + jnp.where(lane > 0, pltpu.roll(near, 1, 1), 0.0)
        total = total + pltpu.roll(met_end, LANES - 2 * SIDE, 1)
        return total * pltpu.roll(met_end, LANES - 3 * SIDE, 1)

    seen = [moved(seen[side], shown[side]) for side in range(2)]
    borders(first_of, store_first, seen, 0)
    sweep(first_of, inverse_of, store_second)

    def step(x):
        for y in range(SIDE):
            pack(FINAL + x * SIDE + y, second_of, x, y)
    spread(2, step)
    for c in range(SIDE):
        for side in range(2):
            @pl.when(lending(c, side))
            def _():
                lent(c, side).start()

    soon = jnp.where((rank == 1) | (rank == n - 2), SIDE, EARLY)

    def release(early):
        for c in range(SIDE):
            for side in range(2):
                @pl.when(sides[side][0] & jnp.where(across[side], (c >= routed(side, rank)) & early, early == (c < soon)))
                def _():
                    sent(8 + c, side).start()
    release(True)
    keep.wait()
    tallies.wait()
    keep = pltpu.make_async_copy(every, every_s, local_sem.at[1])
    keep.start()
    keep.wait()
    before, after = 0, 0
    for r in range(half):
        before = before + jnp.where(r < place, every_s[r, 0, 0], 0)
        after = after + jnp.where(r > place, every_s[r, 0, 0], 0)
    drift_next = (n - 1 - rank) * AVG - after
    drift_prev = jnp.where(lower, before - rank * AVG, drift_next - held + AVG)
    drift_prev = jnp.clip(drift_prev, -HALF, HALF)
    drift_next = jnp.clip(drift_prev + held - AVG, -HALF, HALF)
    base = lax.shift_right_arithmetic(-drift_prev, 7)
    part = (-drift_prev) & (LANES - 1)
    turn = (LANES - part) & (LANES - 1)
    stay = lane >= part
    shift = HALF - jnp.maximum(drift_prev, 0)
    left_part = shift & (LANES - 1)
    left_turn = (LANES - left_part) & (LANES - 1)
    left_pick = (lane >= left_part) & (shift < LANES)
    shift = -HALF - jnp.minimum(drift_next, 0)
    right_part = shift & (LANES - 1)
    right_turn = (LANES - right_part) & (LANES - 1)
    right_pick = (lane < right_part + jnp.where(shift == 0, LANES, 0)) & (shift >= -LANES)
    is_left = [lane + i * LANES < drift_prev for i in range(WIN)]
    is_right = [lane + i * LANES >= HALF + drift_next for i in range(WIN)]

    def aligned(get, x, y):
        lines = [get(x, y, base + i) for i in range(OWN + 1)]
        return [pltpu.roll(jnp.where(stay, lines[i], lines[i + 1]), turn, 1) for i in range(OWN)]

    def windows(unit):
        low, high = got[0, unit, 0], got[0, unit, 1]
        a = [pltpu.roll(jnp.where(left_pick, low, high), left_turn, 1), pltpu.roll(high, left_turn, 1)]
        low, high = got[1, unit, 0], got[1, unit, 1]
        b = [pltpu.roll(low, right_turn, 1), pltpu.roll(jnp.where(right_pick, high, low), right_turn, 1)]
        return a, b

    def merged(get, x, y, unit):
        lines = aligned(get, x, y)
        a, b = windows(unit)
        for i in range(WIN):
            lines[i] = jnp.where(is_left[i], a[i], lines[i])
            lines[OWN - WIN + i] = jnp.where(is_right[i], b[i], lines[OWN - WIN + i])
        return lines

    def face(b, p):
        src, dst = ((face0, near0), (face1, near1))[b]
        return pltpu.make_async_remote_copy(
            src_ref=src.at[p], dst_ref=dst.at[1 - p], send_sem=face_send.at[2 * b + p],
            recv_sem=face_recv.at[2 * b + p], device_id=sides[2 + p][1], device_id_type=MESH,
        )

    def edge(side, p):
        return pltpu.make_async_remote_copy(
            src_ref=edge_out.at[side, p], dst_ref=edge_in.at[1 - side, p], send_sem=edge_send.at[2 * side + p],
            recv_sem=edge_recv.at[2 * side + p], device_id=sides[side][1], device_id_type=MESH,
        )

    for p in range(2):
        arrived(p)
        @pl.when(theres[p])
        def _():
            def step(x):
                lines = merged(field_of, x, outer[p], FIELD + p * SIDE + x)
                for i in range(OWN):
                    face0[p, x, i] = lines[i]
            spread(4, step)
            face(0, p).start()
    for p in range(2):
        arrived(2 + p)
        @pl.when(theres[p])
        def _():
            def step(x):
                lines = merged(inverse_of, x, outer[p], FACTOR + p * SIDE + x)
                for i in range(OWN):
                    inv[p, x, i] = lines[i]
            spread(4, step)

        @pl.when(jnp.logical_not(theres[p]))
        def _():
            @pl.loop(0, SIDE)
            def _(x):
                for k in range(2):
                    for i in range(OWN):
                        change[p, k, x, i] = jnp.zeros((SIDE, LANES), jnp.float32)
    for p in range(2):
        @pl.when(theres[p])
        def _():
            face(0, 1 - p).wait_recv()
            @pl.loop(0, SIDE)
            def _(x):
                for i in range(OWN):
                    value = near0[p, x, i] * inv[p, x, i]
                    fix[p, x + 1, i] = value
            turned = [pltpu.roll(fix[p, 1, i], LANES - 1, 1) for i in range(OWN)]
            edge_out[0, p] = turned[0]
            for i in range(OWN):
                fix[p, SIDE + 1, i] = jnp.where(lane == LANES - 1, turned[i + 1] if i + 1 < OWN else 0.0, turned[i])
            turned = [pltpu.roll(fix[p, SIDE, i], 1, 1) for i in range(OWN)]
            edge_out[1, p] = turned[OWN - 1]
            for i in range(OWN):
                fix[p, 0, i] = jnp.where(lane == 0, turned[i - 1] if i else 0.0, turned[i])
            for side in range(2):
                @pl.when(sides[side][0])
                def _():
                    edge(side, p).start()
    for p in range(2):
        arrived(4 + p)
        @pl.when(theres[p])
        def _():
            def step(x):
                lines = merged(first_of, x, outer[p], MIDDLE + p * SIDE + x)
                for i in range(OWN):
                    face1[p, x, i] = lines[i] + fix[p, x + 1, i]
            spread(4, step)
            face(1, p).start()
    release(False)
    for p in range(2):
        @pl.when(theres[p])
        def _():
            face(1, 1 - p).wait_recv()
            @pl.loop(0, SIDE)
            def _(x):
                for i in range(OWN):
                    total = near1[p, x, i] + (fix[p, x, i] + fix[p, x + 2, i]) + sums(fix[p, x + 1, i])
                    change[p, 0, x, i] = total * inv[p, x, i]
    for p in range(2):
        arrived(6 + p)
        @pl.when(theres[p])
        def _():
            def step(x):
                lines = merged(inverse_of, x, inner[p], FACTOR + (2 + p) * SIDE + x)
                for i in range(OWN):
                    change[p, 1, x, i] = lines[i] * fix[p, x + 1, i]
            spread(4, step)
    for c in range(SIDE):
        for side in range(2):
            @pl.when(passing(c, side))
            def _():
                lent(c, side).wait_recv()
                passed(c, side).start()

    def at(x, y, i):
        return pl.ds((x * SIDE + y) * (SIDE * OWN) + i, SIDE, stride=OWN)

    spots = {0: (0, 0), 1: (0, 1), SIDE - 2: (1, 1), SIDE - 1: (1, 0)}
    window = [i for i in range(OWN) if i < WIN or i >= OWN - WIN]

    @pl.loop(0, SIDE)
    def _(x):
        for y in range(SIDE):
            lines = aligned(second_of, x, y)
            for i in range(OWN):
                if i in window:
                    kept[x, y, window.index(i)] = lines[i]
                elif y in spots:
                    out[at(x, y, i), :] = lines[i] + change[spots[y][0], spots[y][1], x, i]
                else:
                    out[at(x, y, i), :] = lines[i]
    def settle():
        for p in range(2):
            for side, x, i, spot in ((0, 0, 0, 0), (1, SIDE - 1, OWN - 1, LANES - 1)):
                @pl.when(theres[p] & sides[side][0])
                def _():
                    edge(1 - side, p).wait_recv()
                    value = jnp.where(lane == spot, edge_in[side, p] * inv[p, x, i], 0.0)
                    change[p, 0, x, i] = change[p, 0, x, i] + value

    for x in (1, 2, 3, 4, 5, 6, 0, 7):
        if x == 0:
            settle()
        arrived(8 + x)
        for y in range(SIDE):
            a, b = windows(FINAL + x * SIDE + y)
            for j, i in enumerate(window):
                value = jnp.where(is_left[i], a[i], kept[x, y, j]) if i < WIN else jnp.where(
                    is_right[j - WIN], b[j - WIN], kept[x, y, j]
                )
                if y in spots:
                    value = value + change[spots[y][0], spots[y][1], x, i]
                out[at(x, y, i), :] = value
    for side in range(2):
        @pl.when(passes[side])
        def _():
            greeted_on(side).wait_send()

        for c in range(SIDE):
            @pl.when(passing(c, side))
            def _():
                passed(c, side).wait_send()

        @pl.when(sides[side][0])
        def _():
            greeted(side).wait_send()
    for p in range(2):
        @pl.when(theres[p])
        def _():
            for b in range(2):
                face(b, p).wait_send()
            for side in range(2):
                @pl.when(sides[side][0])
                def _():
                    edge(side, p).wait_send()
    for side in range(2):
        for group, there in enumerate((has_low, has_high, True)):
            @pl.when(sides[side][0] & there)
            def _():
                leaving(side, group).wait_send()


def local(state, coef, counts):
    n, groups = lax.axis_size("curve"), lax.axis_size("grp")
    cells, cap = state.shape[1], state.shape[3]
    rows = cap // LANES
    plane = SIDE * SIDE * rows
    f32 = jnp.float32
    vmem, hbm, smem = (pl.BlockSpec(memory_space=m) for m in (pltpu.VMEM, pltpu.HBM, pltpu.SMEM))
    tile = (SIDE, LANES)
    shapes = [(cells * rows + 2 * plane, LANES), (cells * rows, LANES), (cells * rows + PAD, LANES)]
    shapes += [(cells * rows + 2 * PAD, LANES), (cells * rows + 2 * plane, LANES), (cells * rows + 2 * PAD, LANES)]
    shapes += [(2, UNITS, WIN) + tile] * 2
    shapes += [(2, SIDE, OWN) + tile] * 4
    shapes += [(2, SIDE, OWN) + tile, (2, SIDE + 2, OWN) + tile, (2, 2, SIDE, OWN) + tile]
    shapes += [(SIDE, SIDE, 2 * WIN) + tile] + [(2, 2) + tile] * 2
    out = pl.pallas_call(
        functools.partial(exchange, n, groups, rows),
        out_shape=jax.ShapeDtypeStruct((cells * OWN, LANES), f32),
        in_specs=[smem, hbm, hbm],
        out_specs=vmem,
        scratch_shapes=[
            pltpu.VMEM((1, LANES), jnp.int32),
            pltpu.VMEM((n // 2, 1, LANES), jnp.int32),
            pltpu.SMEM((n // 2, 1, LANES), jnp.int32),
            pltpu.VMEM((2,) + tile, f32),
            pltpu.VMEM((2,) + tile, f32),
        ]
        + [pltpu.VMEM(shape, f32) for shape in shapes]
        + [pltpu.SemaphoreType.DMA] * 2
        + [pltpu.SemaphoreType.DMA((k,)) for k in (2, 2, 2, 5, 6, 2 * KINDS, 4, 4, 4, 4)]
        + [pltpu.VMEM(tile, f32)] + [pltpu.SemaphoreType.DMA] * 2
        + [pltpu.VMEM((SIDE, SIDE, WIN) + tile, f32)] + [pltpu.SemaphoreType.DMA((SIDE,))] * 2
        + [pltpu.VMEM((2 * SIDE * SIDE * rows + PAD, LANES), f32)],
        compiler_params=pltpu.CompilerParams(
            collective_id=0, has_side_effects=True, vmem_limit_bytes=50 * 1024 * 1024
        ),
    )(
        counts, state.reshape(2, cells * rows, LANES), coef.reshape(cells * rows, LANES),
    )
    return out.reshape(cells, 1, AVG)


def solution(mesh):
    placed = (P(None, None, "grp", "curve"), P(None, "grp", "curve"), P("grp", "curve"))
    return jax.shard_map(
        local, mesh=mesh, in_specs=placed, out_specs=P(None, "grp", "curve"), check_vma=False
    )
```

```python
import functools

import jax
import jax.numpy as jnp
from jax import lax
from jax.experimental import pallas as pl
from jax.experimental.pallas import tpu as pltpu
from jax.sharding import PartitionSpec as P

AVG = 1024
HALF = 256
LANES = 128
SIDE = 8
WIN = HALF // LANES
OWN = AVG // LANES
PAD = 16
FIELD, FACTOR, MIDDLE, FINAL = 0, 2 * SIDE, 6 * SIDE, 8 * SIDE
UNITS = 16 * SIDE
KINDS = 8 + SIDE
MESH = pl.DeviceIdType.MESH
EARLY = 3


def exchange(
    n, groups, rows, counts, state, coef, out, mine, every, every_s, ends, met, raw0, raw1, raw2, inverse, first,
    second, put, got, face0, face1, near0, near1, inv, fix, change, kept, edge_out, edge_in, count_send, count_recv,
    end_send, end_recv, local_sem, load_sem, send_sem, recv_sem, face_send, face_recv, edge_send, edge_recv,
    via_end, via_end_send, via_end_recv, via, via_send, via_recv,
    rim,
):
    plane_rows = SIDE * SIDE * rows
    cells_rows = SIDE * plane_rows
    rank, group = lax.axis_index("curve"), lax.axis_index("grp")
    has_left, has_right = rank > 0, rank < n - 1
    has_low, has_high = group > 0, group < groups - 1
    sides = (
        (has_left, {"curve": rank - 1}), (has_right, {"curve": rank + 1}),
        (has_low, {"grp": group - 1}), (has_high, {"grp": group + 1}),
    )
    theres = (has_low, has_high)
    raw = (raw0, raw1, raw2)
    front = (plane_rows, 0, 0)
    band = SIDE * rows
    for p, y in enumerate((0, SIDE - 1)):
        for x in range(SIDE):
            pltpu.make_async_copy(
                state.at[0, pl.ds((x * SIDE + y) * band, band)], rim.at[pl.ds((p * SIDE + x) * band, band)], load_sem.at[3]
            ).start()
    sources = (state.at[0], state.at[1], coef)

    def load(f, x, count, sem):
        return pltpu.make_async_copy(
            sources[f].at[pl.ds(x * plane_rows, count * plane_rows)],
            raw[f].at[pl.ds(front[f] + x * plane_rows, count * plane_rows)], load_sem.at[sem],
        )

    for f, x, count in ((0, 0, 2), (0, SIDE - 2, 2), (1, 0, 1), (1, SIDE - 1, 1), (2, 0, 1), (2, SIDE - 1, 1)):
        load(f, x, count, 4).start()
    loads = {0: load(0, 2, SIDE - 4, 0), 2: load(2, 1, SIDE - 2, 2), 1: load(1, 1, SIDE - 2, 1)}
    for f in (2, 0, 1):
        loads[f].start()
    barrier = pltpu.get_barrier_semaphore()
    for there, device in sides[2:]:
        @pl.when(there)
        def _():
            pl.semaphore_signal(barrier, inc=1, device_id=device, device_id_type=MESH)
    half = n // 2
    lower = rank < half
    base_rank = jnp.where(lower, 0, half)
    place = rank - base_rank
    mates = [base_rank + lax.rem(place + off, half) for off in range(1, half)]
    asked = half - 1
    for peer in mates:
        pl.semaphore_signal(barrier, inc=1, device_id={"curve": peer}, device_id_type=MESH)
    for there, device in sides[2:]:
        asked = asked + there.astype(jnp.int32)
    for off in (-2, -1, 1, 2):
        peer = rank + off
        there = (peer >= 0) & (peer < n) & (lower != (peer < half))
        asked = asked + there.astype(jnp.int32)
        @pl.when(there)
        def _():
            pl.semaphore_signal(barrier, inc=1, device_id={"curve": peer}, device_id_type=MESH)

    lane = lax.broadcasted_iota(jnp.int32, (SIDE, LANES), 1)
    level = lax.broadcasted_iota(jnp.int32, (SIDE, LANES), 0)
    held = jnp.clip(counts[0, 0], 2 * HALF, rows * LANES)
    mine[...] = jnp.full((1, LANES), held, jnp.int32)
    last = held - 1
    last_row, last_lane = lax.shift_right_logical(last, 7), last & (LANES - 1)
    tail_row = lax.shift_right_logical(held, 7) - WIN
    tail_part = held & (LANES - 1)
    tail_turn = (LANES - tail_part) & (LANES - 1)
    tail_stay = lane >= tail_part

    def raw_at(f, x, y, r):
        return pl.ds(front[f] + (x * SIDE + y) * (SIDE * rows) + r, SIDE, stride=rows)

    def field_of(x, y, r):
        return raw0[raw_at(0, x, y, r), :]

    def first_at(x, y, r):
        return pl.ds((((x + 1) * SIDE + y) * rows + r) * SIDE, SIDE)

    def flat_at(x, y, r):
        return pl.ds(PAD + ((x * SIDE + y) * rows + r) * SIDE, SIDE)

    def factor_of(x, y, r):
        return 1.0 / (raw2[raw_at(2, x, y, r), :] + 6.0)

    def pack(unit, get, x, y):
        for i in range(WIN):
            put[0, unit, i] = get(x, y, i)
        lines = [get(x, y, tail_row + i) for i in range(WIN + 1)]
        for i in range(WIN):
            put[1, unit, i] = pltpu.roll(jnp.where(tail_stay, lines[i], lines[i + 1]), tail_turn, 1)

    def message(kind):
        if kind < 2:
            return FIELD + kind * SIDE, SIDE
        if kind < 4:
            return FACTOR + (kind - 2) * SIDE, SIDE
        if kind < 6:
            return MIDDLE + (kind - 4) * SIDE, SIDE
        if kind < 8:
            return FACTOR + (kind - 4) * SIDE, SIDE
        return FINAL + (kind - 8) * SIDE, SIDE

    def sent(kind, side):
        start, count = message(kind)
        return pltpu.make_async_remote_copy(
            src_ref=put.at[side, pl.ds(start, count)], dst_ref=got.at[1 - side, pl.ds(start, count)],
            send_sem=send_sem.at[3 * side + (kind % 2 if kind < 8 else 2)], recv_sem=recv_sem.at[side * KINDS + kind],
            device_id=sides[side][1], device_id_type=MESH,
        )

    def leaving(side, group):
        units = pl.ds(FINAL, SIDE * SIDE) if group == 2 else pl.ds(0, 4 * SIDE)
        return pltpu.make_async_remote_copy(
            src_ref=put.at[side, units], dst_ref=got.at[1 - side, units], send_sem=send_sem.at[3 * side + group],
            recv_sem=recv_sem.at[side * KINDS], device_id=sides[side][1], device_id_type=MESH,
        )

    def needed(kind, side):
        return sides[side][0] & theres[kind % 2] if kind < 8 else sides[side][0]

    paired = lax.rem(rank, 2) == 1, lax.rem(rank, 2) == 0
    across = [jnp.logical_not(x) for x in paired]
    passes = paired[0] & (rank >= 2), paired[1] & (rank < n - 2)
    beyond = {"curve": rank - 2}, {"curve": rank + 2}
    steps = max(n // 2 - 1, 1)

    def routed(side, owner):
        return (owner if side == 0 else n - 1 - owner) // 2 * (SIDE + 1) // steps

    def lent(c, side):
        start, count = message(6 + c)
        return pltpu.make_async_remote_copy(
            src_ref=put.at[side, pl.ds(start, count)], dst_ref=via.at[c],
            send_sem=send_sem.at[3 * side + min(c, 2)], recv_sem=via_recv.at[c],
            device_id=sides[1 - side][1], device_id_type=MESH,
        )

    def passed(c, side):
        start, count = message(6 + c)
        return pltpu.make_async_remote_copy(
            src_ref=via.at[c], dst_ref=got.at[1 - side, pl.ds(start, count)],
            send_sem=via_send.at[c], recv_sem=recv_sem.at[side * KINDS + 6 + c],
            device_id=beyond[side], device_id_type=MESH,
        )

    def taken(c, side, owner):
        return theres[c] & (routed(side, owner) > SIDE) if c < 2 else c - 2 < routed(side, owner) - 2 * side * (routed(side, owner) > SIDE)

    def lending(c, side):
        return sides[side][0] & across[side] & taken(c, side, rank)

    def passing(c, side):
        return passes[side] & taken(c, side, rank - 1 + 2 * side)

    def send(kind, only=(True, True)):
        for side in range(2):
            @pl.when(needed(kind, side) & only[side])
            def _():
                sent(kind, side).start()

    def arrived(kind):
        for side in range(2):
            @pl.when(needed(kind, side))
            def _():
                sent(kind, 1 - side).wait_recv()

    def spread(step, fn):
        @pl.loop(0, SIDE // step)
        def _(part):
            for at in range(step):
                fn(step * part + at)

    outer, inner = (0, SIDE - 1), (1, SIDE - 2)
    pltpu.make_async_copy(
        state.at[0, pl.ds(0, 2 * SIDE * band)], rim.at[pl.ds(0, 2 * SIDE * band)], load_sem.at[3]
    ).wait()

    def rim_of(x, p, r):
        return rim[pl.ds((p * SIDE + x) * band + r, SIDE, stride=rows), :]

    def step(x):
        for p in range(2):
            pack(FIELD + p * SIDE + x, rim_of, x, p)
    spread(4, step)
    load(0, 0, SIDE, 4).wait()
    picks = [jnp.zeros((SIDE, LANES), jnp.int32) + last_row == r for r in range(rows)]

    def end_of(f, x, y, at):
        value = raw[f][raw_at(f, x, y, at), :]
        if at:
            for r in range(2 * HALF // LANES - 1, at):
                value = jnp.where(picks[r], raw[f][raw_at(f, x, y, r), :], value)
        return 1.0 / (value + 6.0) if f == 2 else value

    for side, at, turn, outer_x, near_x in ((0, 0, 0, 1, 0), (1, rows - 1, LANES - last_lane, SIDE - 2, SIDE - 1)):
        packed = jnp.zeros((SIDE, LANES), jnp.float32)
        for p, (f, x) in enumerate(((0, outer_x), (0, near_x), (1, near_x), (2, near_x))):
            for y in range(SIDE):
                value = end_of(f, x, y, at)
                spot = p * SIDE + y
                value = pltpu.roll(value, (turn + spot) & (LANES - 1), 1)
                packed = jnp.where(lane == spot, value, packed)
        ends[side] = packed

    pl.semaphore_wait(barrier, asked)

    def greeted(side):
        return pltpu.make_async_remote_copy(
            src_ref=ends.at[side], dst_ref=met.at[1 - side], send_sem=end_send.at[side],
            recv_sem=end_recv.at[side], device_id=sides[side][1], device_id_type=MESH,
        )

    def greeted_via(side):
        return pltpu.make_async_remote_copy(
            src_ref=ends.at[side], dst_ref=via_end, send_sem=end_send.at[side],
            recv_sem=via_end_recv, device_id=sides[1 - side][1], device_id_type=MESH,
        )

    def greeted_on(side):
        return pltpu.make_async_remote_copy(
            src_ref=via_end, dst_ref=met.at[1 - side], send_sem=via_end_send,
            recv_sem=end_recv.at[side], device_id=beyond[side], device_id_type=MESH,
        )

    for side in range(2):
        @pl.when(sides[side][0] & across[side])
        def _():
            greeted_via(side).start()
    for side in range(2):
        @pl.when(sides[side][0] & paired[side])
        def _():
            greeted(side).start()
    for peer in mates:
        pltpu.make_async_remote_copy(
            src_ref=mine, dst_ref=every.at[place], send_sem=count_send, recv_sem=count_recv,
            device_id={"curve": peer}, device_id_type=MESH,
        ).start()
    tallies = pltpu.make_async_remote_copy(
        src_ref=every.at[pl.ds(0, half - 1)], dst_ref=every.at[pl.ds(0, half - 1)], send_sem=count_send,
        recv_sem=count_recv, device_id={"curve": mates[0]}, device_id_type=MESH,
    )
    keep = pltpu.make_async_copy(mine, every.at[place], local_sem.at[0])
    keep.start()
    for kind in range(2):
        send(kind)
    for f in (2, 0, 1):
        loads[f].wait()

    def step(x):
        for p in range(2):
            for k, y in enumerate((outer[p], inner[p])):
                pack(FACTOR + (2 * k + p) * SIDE + x, factor_of, x, y)
    spread(4, step)
    for kind in range(2, 4):
        send(kind)

    for side in range(2):
        @pl.when(passes[side])
        def _():
            greeted_via(side).wait_recv()
            greeted_on(side).start()
    for side in range(2):
        @pl.when(sides[side][0])
        def _():
            greeted(1 - side).wait_recv()
    shown = [ends[side] for side in range(2)]
    seen = [jnp.where(sides[side][0], met[side], 0.0) for side in range(2)]

    def sums(value):
        above = jnp.where(level < SIDE - 1, pltpu.roll(value, SIDE - 1, 0), 0.0)
        return above + jnp.where(level > 0, pltpu.roll(value, 1, 0), 0.0)

    def borders(get, store, ghosts, spot):
        def step(y):
            if True:
                turned = [pltpu.roll(get(SIDE - 1, y, r), 1, 1) for r in range(rows)]
                carry = pltpu.roll(ghosts[0], (LANES - spot - y) & (LANES - 1), 1)
                for r in range(rows):
                    store(-1, y, r, jnp.where(lane == 0, carry, turned[r]))
                    carry = turned[r]
                turned = [pltpu.roll(get(0, y, r), LANES - 1, 1) for r in range(rows)]
                ghost = pltpu.roll(ghosts[1], (last_lane + LANES - spot - y) & (LANES - 1), 1)
                for r in range(rows):
                    value = jnp.where(lane == LANES - 1, turned[r + 1], turned[r]) if r + 1 < rows else turned[r]
                    store(SIDE, y, r, jnp.where(lane + r * LANES == last, ghost, value))
        spread(4, step)

    def sweep(get, factor, store):
        @pl.loop(0, SIDE)
        def _(x):
            for r in range(rows):
                line = [get(x, y, r) for y in range(SIDE)]
                for y in range(SIDE):
                    total = (get(x - 1, y, r) + get(x + 1, y, r)) + (raw1[raw_at(1, x, y, r), :] + sums(line[y]))
                    if y > 0:
                        total = total + line[y - 1]
                    if y + 1 < SIDE:
                        total = total + line[y + 1]
                    store(x, y, r, total * factor(x, y, r))

    def store_field(x, y, r, value):
        raw0[raw_at(0, x, y, r), :] = value

    def first_of(x, y, r):
        return first[first_at(x, y, r), :]

    def store_first(x, y, r, value):
        first[first_at(x, y, r), :] = value

    def made_factor(x, y, r):
        value = factor_of(x, y, r)
        inverse[flat_at(x, y, r), :] = value
        return value

    def inverse_of(x, y, r):
        return inverse[flat_at(x, y, r), :]

    def second_of(x, y, r):
        return second[flat_at(x, y, r), :]

    def store_second(x, y, r, value):
        second[flat_at(x, y, r), :] = value

    borders(field_of, store_field, seen, SIDE)
    sweep(field_of, made_factor, store_first)

    def step(x):
        for p in range(2):
            pack(MIDDLE + p * SIDE + x, first_of, x, outer[p])
    spread(4, step)
    for kind in range(4, 6):
        send(kind)
    for c in range(2):
        for side in range(2):
            @pl.when(lending(c, side))
            def _():
                lent(c, side).start()
    for kind in range(6, 8):
        send(kind, [jnp.logical_not(across[side] & (routed(side, rank) > SIDE)) for side in range(2)])

    def moved(met_end, own_end):
        near = pltpu.roll(met_end, LANES - SIDE, 1)
        total = met_end + pltpu.roll(own_end, LANES - SIDE, 1) + sums(near)
        total = total + jnp.where(lane < SIDE - 1, pltpu.roll(near, LANES - 1, 1), 0.0)
        total = total + jnp.where(lane > 0, pltpu.roll(near, 1, 1), 0.0)
        total = total + pltpu.roll(met_end, LANES - 2 * SIDE, 1)
        return total * pltpu.roll(met_end, LANES - 3 * SIDE, 1)

    seen = [moved(seen[side], shown[side]) for side in range(2)]
    borders(first_of, store_first, seen, 0)
    sweep(first_of, inverse_of, store_second)

    def step(x):
        for y in range(SIDE):
            pack(FINAL + x * SIDE + y, second_of, x, y)
    spread(2, step)
    for c in range(2, SIDE + 2):
        for side in range(2):
            @pl.when(lending(c, side))
            def _():
                lent(c, side).start()

    soon = jnp.where((rank == 1) | (rank == n - 2), SIDE, EARLY)

    def release(early):
        for c in range(SIDE):
            for side in range(2):
                @pl.when(sides[side][0] & jnp.where(across[side], jnp.logical_not(taken(c + 2, side, rank)) & early, early == (c < soon)))
                def _():
                    sent(8 + c, side).start()
    release(True)
    keep.wait()
    tallies.wait()
    keep = pltpu.make_async_copy(every, every_s, local_sem.at[1])
    keep.start()
    keep.wait()
    before, after = 0, 0
    for r in range(half):
        before = before + jnp.where(r < place, every_s[r, 0, 0], 0)
        after = after + jnp.where(r > place, every_s[r, 0, 0], 0)
    drift_next = (n - 1 - rank) * AVG - after
    drift_prev = jnp.where(lower, before - rank * AVG, drift_next - held + AVG)
    drift_prev = jnp.clip(drift_prev, -HALF, HALF)
    drift_next = jnp.clip(drift_prev + held - AVG, -HALF, HALF)
    base = lax.shift_right_arithmetic(-drift_prev, 7)
    part = (-drift_prev) & (LANES - 1)
    turn = (LANES - part) & (LANES - 1)
    stay = lane >= part
    shift = HALF - jnp.maximum(drift_prev, 0)
    left_part = shift & (LANES - 1)
    left_turn = (LANES - left_part) & (LANES - 1)
    left_pick = (lane >= left_part) & (shift < LANES)
    shift = -HALF - jnp.minimum(drift_next, 0)
    right_part = shift & (LANES - 1)
    right_turn = (LANES - right_part) & (LANES - 1)
    right_pick = (lane < right_part + jnp.where(shift == 0, LANES, 0)) & (shift >= -LANES)
    is_left = [lane + i * LANES < drift_prev for i in range(WIN)]
    is_right = [lane + i * LANES >= HALF + drift_next for i in range(WIN)]

    def aligned(get, x, y):
        lines = [get(x, y, base + i) for i in range(OWN + 1)]
        return [pltpu.roll(jnp.where(stay, lines[i], lines[i + 1]), turn, 1) for i in range(OWN)]

    def windows(unit):
        low, high = got[0, unit, 0], got[0, unit, 1]
        a = [pltpu.roll(jnp.where(left_pick, low, high), left_turn, 1), pltpu.roll(high, left_turn, 1)]
        low, high = got[1, unit, 0], got[1, unit, 1]
        b = [pltpu.roll(low, right_turn, 1), pltpu.roll(jnp.where(right_pick, high, low), right_turn, 1)]
        return a, b

    def merged(get, x, y, unit):
        lines = aligned(get, x, y)
        a, b = windows(unit)
        for i in range(WIN):
            lines[i] = jnp.where(is_left[i], a[i], lines[i])
            lines[OWN - WIN + i] = jnp.where(is_right[i], b[i], lines[OWN - WIN + i])
        return lines

    def face(b, p):
        src, dst = ((face0, near0), (face1, near1))[b]
        return pltpu.make_async_remote_copy(
            src_ref=src.at[p], dst_ref=dst.at[1 - p], send_sem=face_send.at[2 * b + p],
            recv_sem=face_recv.at[2 * b + p], device_id=sides[2 + p][1], device_id_type=MESH,
        )

    def edge(side, p):
        return pltpu.make_async_remote_copy(
            src_ref=edge_out.at[side, p], dst_ref=edge_in.at[1 - side, p], send_sem=edge_send.at[2 * side + p],
            recv_sem=edge_recv.at[2 * side + p], device_id=sides[side][1], device_id_type=MESH,
        )

    for p in range(2):
        arrived(p)
        @pl.when(theres[p])
        def _():
            def step(x):
                lines = merged(field_of, x, outer[p], FIELD + p * SIDE + x)
                for i in range(OWN):
                    face0[p, x, i] = lines[i]
            spread(4, step)
            face(0, p).start()
    for p in range(2):
        arrived(2 + p)
        @pl.when(theres[p])
        def _():
            def step(x):
                lines = merged(inverse_of, x, outer[p], FACTOR + p * SIDE + x)
                for i in range(OWN):
                    inv[p, x, i] = lines[i]
            spread(4, step)

        @pl.when(jnp.logical_not(theres[p]))
        def _():
            @pl.loop(0, SIDE)
            def _(x):
                for k in range(2):
                    for i in range(OWN):
                        change[p, k, x, i] = jnp.zeros((SIDE, LANES), jnp.float32)
    for p in range(2):
        @pl.when(theres[p])
        def _():
            face(0, 1 - p).wait_recv()
            @pl.loop(0, SIDE)
            def _(x):
                for i in range(OWN):
                    value = near0[p, x, i] * inv[p, x, i]
                    fix[p, x + 1, i] = value
            turned = [pltpu.roll(fix[p, 1, i], LANES - 1, 1) for i in range(OWN)]
            edge_out[0, p] = turned[0]
            for i in range(OWN):
                fix[p, SIDE + 1, i] = jnp.where(lane == LANES - 1, turned[i + 1] if i + 1 < OWN else 0.0, turned[i])
            turned = [pltpu.roll(fix[p, SIDE, i], 1, 1) for i in range(OWN)]
            edge_out[1, p] = turned[OWN - 1]
            for i in range(OWN):
                fix[p, 0, i] = jnp.where(lane == 0, turned[i - 1] if i else 0.0, turned[i])
            for side in range(2):
                @pl.when(sides[side][0])
                def _():
                    edge(side, p).start()
    for p in range(2):
        arrived(4 + p)
        @pl.when(theres[p])
        def _():
            def step(x):
                lines = merged(first_of, x, outer[p], MIDDLE + p * SIDE + x)
                for i in range(OWN):
                    face1[p, x, i] = lines[i] + fix[p, x + 1, i]
            spread(4, step)
            face(1, p).start()
    release(False)
    for p in range(2):
        @pl.when(theres[p])
        def _():
            face(1, 1 - p).wait_recv()
            @pl.loop(0, SIDE)
            def _(x):
                for i in range(OWN):
                    total = near1[p, x, i] + (fix[p, x, i] + fix[p, x + 2, i]) + sums(fix[p, x + 1, i])
                    change[p, 0, x, i] = total * inv[p, x, i]
    for p in range(2):
        arrived(6 + p)
        @pl.when(theres[p])
        def _():
            def step(x):
                lines = merged(inverse_of, x, inner[p], FACTOR + (2 + p) * SIDE + x)
                for i in range(OWN):
                    change[p, 1, x, i] = lines[i] * fix[p, x + 1, i]
            spread(4, step)
    for c in range(SIDE + 2):
        for side in range(2):
            @pl.when(passing(c, side))
            def _():
                lent(c, side).wait_recv()
                passed(c, side).start()

    def at(x, y, i):
        return pl.ds((x * SIDE + y) * (SIDE * OWN) + i, SIDE, stride=OWN)

    spots = {0: (0, 0), 1: (0, 1), SIDE - 2: (1, 1), SIDE - 1: (1, 0)}
    window = [i for i in range(OWN) if i < WIN or i >= OWN - WIN]

    @pl.loop(0, SIDE)
    def _(x):
        for y in range(SIDE):
            lines = aligned(second_of, x, y)
            for i in range(OWN):
                if i in window:
                    kept[x, y, window.index(i)] = lines[i]
                elif y in spots:
                    out[at(x, y, i), :] = lines[i] + change[spots[y][0], spots[y][1], x, i]
                else:
                    out[at(x, y, i), :] = lines[i]
    def settle():
        for p in range(2):
            for side, x, i, spot in ((0, 0, 0, 0), (1, SIDE - 1, OWN - 1, LANES - 1)):
                @pl.when(theres[p] & sides[side][0])
                def _():
                    edge(1 - side, p).wait_recv()
                    value = jnp.where(lane == spot, edge_in[side, p] * inv[p, x, i], 0.0)
                    change[p, 0, x, i] = change[p, 0, x, i] + value

    for x in (1, 2, 3, 4, 5, 6, 0, 7):
        if x == 0:
            settle()
        arrived(8 + x)
        for y in range(SIDE):
            a, b = windows(FINAL + x * SIDE + y)
            for j, i in enumerate(window):
                value = jnp.where(is_left[i], a[i], kept[x, y, j]) if i < WIN else jnp.where(
                    is_right[j - WIN], b[j - WIN], kept[x, y, j]
                )
                if y in spots:
                    value = value + change[spots[y][0], spots[y][1], x, i]
                out[at(x, y, i), :] = value
    for side in range(2):
        @pl.when(passes[side])
        def _():
            greeted_on(side).wait_send()

        for c in range(SIDE + 2):
            @pl.when(passing(c, side))
            def _():
                passed(c, side).wait_send()

        @pl.when(sides[side][0])
        def _():
            greeted(side).wait_send()
    for p in range(2):
        @pl.when(theres[p])
        def _():
            for b in range(2):
                face(b, p).wait_send()
            for side in range(2):
                @pl.when(sides[side][0])
                def _():
                    edge(side, p).wait_send()
    for side in range(2):
        for group, there in enumerate((has_low, has_high, True)):
            @pl.when(sides[side][0] & there)
            def _():
                leaving(side, group).wait_send()


def local(state, coef, counts):
    n, groups = lax.axis_size("curve"), lax.axis_size("grp")
    cells, cap = state.shape[1], state.shape[3]
    rows = cap // LANES
    plane = SIDE * SIDE * rows
    f32 = jnp.float32
    vmem, hbm, smem = (pl.BlockSpec(memory_space=m) for m in (pltpu.VMEM, pltpu.HBM, pltpu.SMEM))
    tile = (SIDE, LANES)
    shapes = [(cells * rows + 2 * plane, LANES), (cells * rows, LANES), (cells * rows + PAD, LANES)]
    shapes += [(cells * rows + 2 * PAD, LANES), (cells * rows + 2 * plane, LANES), (cells * rows + 2 * PAD, LANES)]
    shapes += [(2, UNITS, WIN) + tile] * 2
    shapes += [(2, SIDE, OWN) + tile] * 4
    shapes += [(2, SIDE, OWN) + tile, (2, SIDE + 2, OWN) + tile, (2, 2, SIDE, OWN) + tile]
    shapes += [(SIDE, SIDE, 2 * WIN) + tile] + [(2, 2) + tile] * 2
    out = pl.pallas_call(
        functools.partial(exchange, n, groups, rows),
        out_shape=jax.ShapeDtypeStruct((cells * OWN, LANES), f32),
        in_specs=[smem, hbm, hbm],
        out_specs=vmem,
        scratch_shapes=[
            pltpu.VMEM((1, LANES), jnp.int32),
            pltpu.VMEM((n // 2, 1, LANES), jnp.int32),
            pltpu.SMEM((n // 2, 1, LANES), jnp.int32),
            pltpu.VMEM((2,) + tile, f32),
            pltpu.VMEM((2,) + tile, f32),
        ]
        + [pltpu.VMEM(shape, f32) for shape in shapes]
        + [pltpu.SemaphoreType.DMA] * 2
        + [pltpu.SemaphoreType.DMA((k,)) for k in (2, 2, 2, 5, 6, 2 * KINDS, 4, 4, 4, 4)]
        + [pltpu.VMEM(tile, f32)] + [pltpu.SemaphoreType.DMA] * 2
        + [pltpu.VMEM((SIDE + 2, SIDE, WIN) + tile, f32)] + [pltpu.SemaphoreType.DMA((SIDE + 2,))] * 2
        + [pltpu.VMEM((2 * SIDE * SIDE * rows + PAD, LANES), f32)],
        compiler_params=pltpu.CompilerParams(
            collective_id=0, has_side_effects=True, vmem_limit_bytes=50 * 1024 * 1024
        ),
    )(
        counts, state.reshape(2, cells * rows, LANES), coef.reshape(cells * rows, LANES),
    )
    return out.reshape(cells, 1, AVG)


def solution(mesh):
    placed = (P(None, None, "grp", "curve"), P(None, "grp", "curve"), P("grp", "curve"))
    return jax.shard_map(
        local, mesh=mesh, in_specs=placed, out_specs=P(None, "grp", "curve"), check_vma=False
    )
```
